32 devices in a mesh: shard: 4 (over x, core), context: 2 (over y), tensor: 4 (over z).
Axes of the slice: x: 2, y: 2, z: 4, core: 2. Of those that a mesh axis runs over, the one named last changes fastest.
Arguments:
- hidden: bfloat16 [4, 1024, 2048], P('shard', 'context'), may hold values from -6 to 6
- norm1_gain: float32 [2048], replicated, may hold values from 0.5 to 1.5
- w_query: bfloat16 [2048, 2048], P('shard', 'tensor'), may hold values from -0.125 to 0.125
- w_key: bfloat16 [2048, 2048], P('shard', 'tensor'), may hold values from -0.125 to 0.125
- w_value: bfloat16 [2048, 2048], P('shard', 'tensor'), may hold values from -0.125 to 0.125
- query_gain: float32 [2048], P('tensor'), may hold values from 0.5 to 1.5
- key_gain: float32 [2048], P('tensor'), may hold values from 0.5 to 1.5
- w_output: bfloat16 [2048, 2048], P('tensor', 'shard'), may hold values from -0.5 to 0.5
- norm2_gain: float32 [2048], replicated, may hold values from 0.5 to 1.5
- w_router: bfloat16 [2048, 16], P('shard'), may hold values from -0.125 to 0.125
- w_gate: bfloat16 [16, 2048, 1024], P(None, 'shard', 'tensor'), may hold values from -0.125 to 0.125
- w_up: bfloat16 [16, 2048, 1024], P(None, 'shard', 'tensor'), may hold values from -0.125 to 0.125
- w_down: bfloat16 [16, 1024, 2048], P(None, 'tensor', 'shard'), may hold values from -1.5 to 1.5
- seq_lengths: int32 [4], P('shard'), may hold values from 256 to 1024, as said below
- expert_routes: int32 [4, 1024, 8], P('shard', 'context'), may hold values from 0 to 15, all different within a row
- out_grad: bfloat16 [4, 1024, 2048], P('shard', 'context'), may hold values from -6 to 6
Outputs:
- block_out: bfloat16 [4, 1024, 2048], P('shard', 'context')
- input_grad: bfloat16 [4, 1024, 2048], P('shard', 'context')
- norm1_gain_grad: float32 [2048], replicated
- w_query_grad: float32 [2048, 2048], P('shard', 'tensor')
- w_key_grad: float32 [2048, 2048], P('shard', 'tensor')
- w_value_grad: float32 [2048, 2048], P('shard', 'tensor')
- query_gain_grad: float32 [2048], P('tensor')
- key_gain_grad: float32 [2048], P('tensor')
- w_output_grad: float32 [2048, 2048], P('tensor', 'shard')
- norm2_gain_grad: float32 [2048], replicated
- w_router_grad: float32 [2048, 16], P('shard')
- w_gate_grad: float32 [16, 2048, 1024], P(None, 'shard', 'tensor')
- w_up_grad: float32 [16, 2048, 1024], P(None, 'shard', 'tensor')
- w_down_grad: float32 [16, 1024, 2048], P(None, 'tensor', 'shard')
The draws below stay inside these ranges and needn't reach their ends.
Inputs may be any that keep to these rules, and one draw needn't show every extreme that they name: `seq_lengths`: each slot's valid positions come first; some slot has all 1024 in every draw. `expert_routes`: each position names 8 different experts.
All inputs are finite; a program needn't handle non-finite values.
Results may differ from the reference program's by a relative error of at most 0.018.
Values may be sent and summed in bfloat16 or wider, within the bound.
A program may use at most 320 MiB of HBM per device.

```python
import math
import jax
import jax.numpy as jnp
from jax import lax

D = 2048
HEADS = 16
HEAD_DIM = 128
FF = 1024
EXPERTS = 16
TOPK = 8
LENGTH = 1024
SLOTS = 4


def draw_seq_lengths(key, part):
    key_len, key_pick = jax.random.split(jax.random.fold_in(key, 7))
    drawn_len = jax.random.randint(key_len, (SLOTS,), LENGTH // 4, LENGTH + 1)
    chosen = jax.random.randint(key_pick, (), 0, SLOTS)
    return jnp.where(jnp.arange(SLOTS) == chosen, LENGTH, drawn_len).astype(jnp.int32)


def block_scale(own_key, extent, cuts, smallest, top_value):
    level, own = 1.0, jax.random.fold_in(own_key, 6)
    for dim, parts in cuts:
        steps = jnp.exp(jax.random.uniform(jax.random.fold_in(own, dim), (parts,), jnp.float32, smallest / len(cuts), top_value / len(cuts)))
        level = level * jnp.repeat(steps, extent[dim] // parts).reshape([-1 if axis == dim else 1 for axis in range(len(extent))])
    return level


def distinct(key, rows, count, top, lift):
    ranking = jax.random.permutation(jax.random.fold_in(key, 1), count)
    pull = ranking
    for power in range(3):
        pull = pull * pull // count
    pull = pull * lift // count
    tickets = jax.random.randint(jax.random.fold_in(key, 2), (rows, count), 0, 4096) + pull
    sure = jax.random.permutation(jax.random.fold_in(key, 3), rows)[jnp.arange(count) % rows]
    tickets = jnp.where(jnp.arange(rows)[:, None] == sure[None, :], 1 << 14, tickets)
    score = tickets * count + jnp.arange(count)
    return lax.top_k(score.astype(jnp.int32), top)[1].astype(jnp.int32)


def normal_values(stream_key, shape, width, limit, cuts=(), held_as=jnp.bfloat16):
    gain = block_scale(stream_key, shape, cuts, -0.22, 0.18) if cuts else 1.0
    entries = jax.random.normal(stream_key, shape, jnp.float32) * width * gain
    return jnp.minimum(jnp.maximum(entries, -limit), limit).astype(held_as)


def setup_inputs(seed: int = 0) -> dict:
    arg_keys = jax.random.split(jax.random.key(seed), 17)
    return {
        "hidden": normal_values(arg_keys[0], (SLOTS, LENGTH, D), 1.0, 6.0, ((0, 4), (1, 2))),
        "norm1_gain": jnp.clip(1.0 + 0.1 * jax.random.normal(arg_keys[1], (D,), jnp.float32), 0.5, 1.5),
        "w_query": normal_values(arg_keys[2], (D, D), D ** -0.5, 0.125, ((0, 4), (1, 4))),
        "w_key": normal_values(arg_keys[3], (D, D), D ** -0.5, 0.125, ((0, 4), (1, 4))),
        "w_value": normal_values(arg_keys[4], (D, D), D ** -0.5, 0.125, ((0, 4), (1, 4))),
        "query_gain": jnp.clip(1.0 + 0.1 * jax.random.normal(arg_keys[5], (D,), jnp.float32), 0.5, 1.5),
        "key_gain": jnp.clip(1.0 + 0.1 * jax.random.normal(arg_keys[6], (D,), jnp.float32), 0.5, 1.5),
        "w_output": normal_values(arg_keys[7], (D, D), (D // 16) ** -0.5, 0.5, ((0, 4), (1, 4))),
        "norm2_gain": jnp.clip(1.0 + 0.1 * jax.random.normal(arg_keys[8], (D,), jnp.float32), 0.5, 1.5),
        "w_router": normal_values(arg_keys[9], (D, EXPERTS), D ** -0.5, 0.125, ((0, 4),)),
        "w_gate": normal_values(arg_keys[10], (EXPERTS, D, FF), D ** -0.5, 0.125, ((1, 4), (2, 4))),
        "w_up": normal_values(arg_keys[11], (EXPERTS, D, FF), D ** -0.5, 0.125, ((1, 4), (2, 4))),
        "w_down": normal_values(arg_keys[12], (EXPERTS, FF, D), (max(FF // 64, 1)) ** -0.5, 1.5, ((1, 4), (2, 4))),
        "seq_lengths": draw_seq_lengths(jax.random.fold_in(arg_keys[16], 71), 0),
        "expert_routes": distinct(arg_keys[14], SLOTS * LENGTH, EXPERTS, TOPK, 4096).reshape((SLOTS, LENGTH, TOPK)),
        "out_grad": normal_values(arg_keys[15], (SLOTS, LENGTH, D), 1.0, 6.0, ((0, 4), (1, 2))),
    }


@jax.custom_vjp
def low(v):
    return lax.optimization_barrier(v.astype(jnp.bfloat16)).astype(jnp.float32)

@jax.custom_vjp
def low_back(v):
    return v

def low_keep(v):
    return (low(v), None)

def low_pass(kept, grad):
    return (grad,)

def back_keep(v):
    return (v, None)

def back_low(kept, grad):
    return (low(grad),)
low.defvjp(low_keep, low_pass)
low_back.defvjp(back_keep, back_low)
EPSILON = 1e-05
HIGHEST = lax.Precision.HIGHEST

def matmul_high(left_side, right_side):
    return jnp.dot(left_side, right_side, precision=HIGHEST)

def rms_norm(values, gain_vec):
    return values * lax.rsqrt(lax.optimization_barrier(jnp.mean(values * values, axis=-1, keepdims=True)) + EPSILON) * gain_vec

def rotate(field, cosine, sine_part):
    half_dim = field.shape[-1] // 2
    first_half = field[..., :half_dim]
    second_half = field[..., half_dim:]
    return jnp.concatenate([first_half * cosine - second_half * sine_part, second_half * cosine + first_half * sine_part], axis=-1)

def attention(query_rot, key_rot, value_all):
    seq_len = query_rot.shape[0]
    block_rows = math.gcd(seq_len, 512)
    block_count = seq_len // block_rows
    key_pos = jnp.arange(seq_len, dtype=jnp.int32)

    def score_block(pieces):
        query_block, start_row = pieces
        query_pos = start_row + jnp.arange(block_rows, dtype=jnp.int32)
        raw_scores = jnp.einsum('qhc,khc->hqk', query_block, key_rot, precision=HIGHEST) * HEAD_DIM ** (-0.5)
        raw_scores = low_back(raw_scores)
        masked = jnp.where(key_pos[None, None, :] <= query_pos[None, :, None], raw_scores, -1e+30)
        top_score = lax.optimization_barrier(jnp.max(masked, axis=-1, keepdims=True))
        expo_vals = jnp.exp(masked - top_score)
        attn_probs = expo_vals / lax.optimization_barrier(jnp.sum(expo_vals, axis=-1, keepdims=True))
        return jnp.einsum('hqk,khc->qhc', low(attn_probs), value_all, precision=HIGHEST)
    start_rows = jnp.arange(block_count, dtype=jnp.int32) * block_rows
    blocks_out = lax.map(jax.checkpoint(score_block), (query_rot.reshape(block_count, block_rows, HEADS, HEAD_DIM), start_rows))
    return blocks_out.reshape(seq_len, HEADS, HEAD_DIM)

def block_forward(weights_all, resid_in, valid_rows, member):
    norm1_gain, w_query, w_key, w_value, query_gain, key_gain, w_output, norm2_gain, w_router, w_gate, w_up, w_down = weights_all
    seq_len = resid_in.shape[0]
    normed_one = low(rms_norm(resid_in, norm1_gain))
    query_proj = low_back(matmul_high(normed_one, w_query))
    key_proj = low_back(matmul_high(normed_one, w_key))
    value_proj = low_back(low(matmul_high(normed_one, w_value)))
    query_norm = rms_norm(query_proj, query_gain)
    key_norm = rms_norm(key_proj, key_gain)
    half_dim = HEAD_DIM // 2
    inv_freq = 10000.0 ** (-(2.0 * jnp.arange(half_dim, dtype=jnp.float32)) / HEAD_DIM)
    angles = jnp.arange(seq_len, dtype=jnp.float32)[:, None] * inv_freq[None, :]
    cosine = jnp.cos(angles)[:, None, :]
    sine_part = jnp.sin(angles)[:, None, :]
    query_rot = low(rotate(query_norm.reshape(seq_len, HEADS, HEAD_DIM), cosine, sine_part))
    key_rot = low(rotate(key_norm.reshape(seq_len, HEADS, HEAD_DIM), cosine, sine_part))
    mixed_heads = low_back(low(attention(query_rot, key_rot, value_proj.reshape(seq_len, HEADS, HEAD_DIM)))).reshape(seq_len, D)
    attn_out = low_back(matmul_high(mixed_heads, w_output))
    resid_mid = resid_in + attn_out
    normed_two = low(rms_norm(resid_mid, norm2_gain))
    logits = low_back(matmul_high(normed_two, w_router))
    top_logit = lax.optimization_barrier(jnp.max(logits, axis=-1, keepdims=True))
    expo_logit = jnp.exp(logits - top_logit)
    router = expo_logit / lax.optimization_barrier(jnp.sum(expo_logit, axis=-1, keepdims=True))
    coef_all = router * member

    def expert_step(running, pieces):
        gate_w, up_w, down_w, weight_col = pieces
        gate_proj = low_back(matmul_high(normed_two, gate_w))
        up_proj = low_back(matmul_high(normed_two, up_w))
        inner_act = low(jax.nn.silu(gate_proj) * up_proj)
        expert_out = low_back(matmul_high(inner_act, down_w))
        return (running + weight_col[:, None] * expert_out, None)
    moe_out, unused = lax.scan(jax.checkpoint(expert_step), jnp.zeros((seq_len, D), jnp.float32), (w_gate, w_up, w_down, coef_all.T))
    return valid_rows[:, None] * (resid_mid + moe_out)

def reference(hidden, norm1_gain, w_query, w_key, w_value, query_gain, key_gain, w_output, norm2_gain, w_router, w_gate, w_up, w_down, seq_lengths, expert_routes, out_grad):
    weights_all = tuple((array_in.astype(jnp.float32) for array_in in (norm1_gain, w_query, w_key, w_value, query_gain, key_gain, w_output, norm2_gain, w_router, w_gate, w_up, w_down)))
    expert_ids = jnp.arange(EXPERTS, dtype=jnp.int32)
    positions = jnp.arange(LENGTH, dtype=jnp.int32)

    def per_slot(grad_totals, inputs):
        resid_in, slot_len, routes, cotangent = inputs
        valid_rows = (positions < slot_len).astype(jnp.float32)
        member = jnp.any(routes[:, :, None] == expert_ids[None, None, :], axis=1).astype(jnp.float32)

        def forward(weights_now, resid_now):
            return block_forward(weights_now, resid_now, valid_rows, member)
        out_now, pullback = jax.vjp(forward, weights_all, resid_in.astype(jnp.float32))
        weight_grads, input_now = pullback(cotangent.astype(jnp.float32))
        grad_totals = jax.tree.map(jnp.add, grad_totals, weight_grads)
        return (grad_totals, (out_now.astype(jnp.bfloat16), input_now.astype(jnp.bfloat16)))
    zero_grads = tuple((jnp.zeros(array_in.shape, jnp.float32) for array_in in weights_all))
    grad_totals, (block_out, input_grad) = lax.scan(per_slot, zero_grads, (hidden, seq_lengths, expert_routes, out_grad))
    grad_norm1, grad_query, grad_key, grad_value, grad_qgain, grad_kgain, grad_output, grad_norm2, grad_router, grad_gate, grad_up, grad_down = grad_totals
    return (block_out, input_grad, grad_norm1, grad_query, grad_key, grad_value, grad_qgain, grad_kgain, grad_output, grad_norm2, grad_router, grad_gate, grad_up, grad_down)
```

```python
import functools

import jax
import jax.numpy as jnp
from jax import lax
from jax.experimental import pallas as pl
from jax.experimental.pallas import tpu as pltpu
from jax.sharding import PartitionSpec as P

HEAD_DIM = 128
EPSILON = 1e-05
GROUP = 4
f32 = jnp.float32
bf16 = jnp.bfloat16


def nn(a, b):
    return lax.dot_general(a, b, (((1,), (0,)), ((), ())), preferred_element_type=f32)


def nt(a, b):
    return lax.dot_general(a, b, (((1,), (1,)), ((), ())), preferred_element_type=f32)


def tn(a, b):
    return lax.dot_general(a, b, (((0,), (0,)), ((), ())), preferred_element_type=f32)


def moe_kernel(
    first, count, order,
    h_ref, ht_ref, g_ref, gt_ref, coef_ref,
    w_own, w_core, x_near, y_near, x_far, y_far,
    moe_in, dh_in, dc_in,
    moe_ref, dh_ref, dc_ref, keep_ref, send_ref,
    wbuf, sems,
):
    step = pl.program_id(0)
    chunk = h_ref.shape[1] // 4
    half = count // 2

    def fetch(at, slot, act):
        expert = order[at]

        def one(src, piece):
            dst = wbuf.at[slot, :, pl.ds(piece * chunk, chunk)]
            act(pltpu.make_async_copy(src, dst, sems.at[slot, piece]))

        one(w_own.at[:, expert], 0)
        one(w_core.at[:, expert], 1)

        @pl.when(at < half)
        def _():
            one(x_near.at[:, at], 2)
            one(x_far.at[:, at], 3)

        @pl.when(at >= half)
        def _():
            one(y_near.at[:, at - half], 2)
            one(y_far.at[:, at - half], 3)

    slot = lax.rem(step, 2)

    @pl.when(step == 0)
    def _():
        fetch(0, 0, lambda c: c.start())
        if first:
            moe_ref[...] = jnp.zeros_like(moe_ref)
            dh_ref[...] = jnp.zeros_like(dh_ref)
            dc_ref[...] = jnp.zeros_like(dc_ref)
        else:
            moe_ref[...] = moe_in[...]
            dh_ref[...] = dh_in[...]
            dc_ref[...] = dc_in[...]

    @pl.when(step + 1 < count)
    def _():
        fetch(step + 1, 1 - slot, lambda c: c.start())

    fetch(step, slot, lambda c: c.wait())
    lanes = lax.broadcasted_iota(jnp.int32, coef_ref.shape, 1)
    picked = lanes == order[step]
    coef = jnp.sum(jnp.where(picked, coef_ref[...], 0.0), axis=1, keepdims=True)
    wg, wu, wd = wbuf.at[slot, 0], wbuf.at[slot, 1], wbuf.at[slot, 2]
    gate = nn(h_ref[...], wg[...])
    up = nn(h_ref[...], wu[...])
    dz_plain = nn(g_ref[...], wd[...])
    sig = jax.nn.sigmoid(gate)
    act = gate * sig
    z = act * up
    z_coef = (z * coef).astype(bf16)
    dcoef = jnp.sum(z * dz_plain, axis=1, keepdims=True)
    dc_ref[...] += jnp.where(picked, dcoef, 0.0)
    dz = dz_plain * coef
    dgate = (dz * up * (sig * (1.0 + gate * (1.0 - sig)))).astype(bf16)
    dup = (dz * act).astype(bf16)
    for j in range(4):
        rows = slice(j * chunk, (j + 1) * chunk)
        moe_ref[:, rows] += nt(z_coef, wd[rows, :])
        dh_ref[:, rows] += nt(dgate, wg[rows, :]) + nt(dup, wu[rows, :])
        out = keep_ref if j % 2 == 0 else send_ref
        out[0, 0, j // 2] = nn(ht_ref[rows, :], dgate).astype(bf16)
        out[1, 0, j // 2] = nn(ht_ref[rows, :], dup).astype(bf16)
        out[2, 0, j // 2] = nn(gt_ref[rows, :], z_coef).astype(bf16)


def moe_call(base, order, h, ht, g, gt, coef, w_own, w_core, xs, sums):
    tokens, width = h.shape
    hidden = w_own.shape[3]
    chunk = width // 4
    first = sums is None
    if first:
        sums = tuple(jnp.zeros((8, 128), f32) for _ in range(3))

    def whole(shape):
        return pl.BlockSpec(
            shape, lambda i, o: (0,) * len(shape), pipeline_mode=pl.Buffered(1)
        )

    anywhere = pl.BlockSpec(memory_space=pl.ANY)
    grad_spec = pl.BlockSpec(
        (3, 1, 2, chunk, hidden), lambda i, o: (0, o[i] - base, 0, 0, 0)
    )
    grad_shape = jax.ShapeDtypeStruct((3, GROUP, 2, chunk, hidden), bf16)
    return pl.pallas_call(
        functools.partial(moe_kernel, first, GROUP),
        grid_spec=pltpu.PrefetchScalarGridSpec(
            num_scalar_prefetch=1,
            grid=(GROUP,),
            in_specs=[whole(a.shape) for a in (h, ht, g, gt, coef)]
            + [anywhere] * 6
            + [whole(a.shape) for a in sums],
            out_specs=[whole(h.shape), whole(h.shape), whole(coef.shape), grad_spec, grad_spec],
            scratch_shapes=[
                pltpu.VMEM((2, 3, width, hidden), bf16),
                pltpu.SemaphoreType.DMA((2, 4)),
            ],
        ),
        out_shape=[
            jax.ShapeDtypeStruct(h.shape, f32),
            jax.ShapeDtypeStruct(h.shape, f32),
            jax.ShapeDtypeStruct(coef.shape, f32),
            grad_shape,
            grad_shape,
        ],
        compiler_params=pltpu.CompilerParams(
            dimension_semantics=("arbitrary",), vmem_limit_bytes=60 * 1024 * 1024
        ),
        cost_estimate=pl.CostEstimate(
            flops=18 * tokens * width * hidden * GROUP,
            bytes_accessed=12 * width * hidden * GROUP + 32 * tokens * width,
            transcendentals=GROUP * tokens * hidden,
        ),
        name="moe_first" if first else "moe_next",
    )(order, h, ht, g, gt, coef, w_own, w_core, *xs, *sums)


def rotate(field, cosine, sine_part):
    half_dim = field.shape[-1] // 2
    a, b = field[..., :half_dim], field[..., half_dim:]
    return jnp.concatenate([a * cosine - b * sine_part, b * cosine + a * sine_part], axis=-1)


def unrotate(field, cosine, sine_part):
    return rotate(field, cosine, -sine_part)


def body(
    hidden, norm1_gain, w_query, w_key, w_value, query_gain, key_gain, w_output,
    norm2_gain, w_router, w_gate, w_up, w_down, seq_lengths, expert_routes, out_grad,
):
    slots, tokens, width = hidden.shape
    shards, contexts, tensors = (
        lax.axis_size("shard"),
        lax.axis_size("context"),
        lax.axis_size("tensor"),
    )
    assert slots == 1 and shards == 4
    me, here, mine = lax.axis_index("shard"), lax.axis_index("context"), lax.axis_index("tensor")
    pair = contexts == 2
    chunk = width // shards
    cols = w_query.shape[1]
    heads = cols // HEAD_DIM
    experts = w_gate.shape[0]
    scale = HEAD_DIM ** (-0.5)
    rows = tokens // tensors

    def to_core(a):
        return lax.ppermute(a, "shard", [(s, s ^ 1) for s in range(shards)])

    def to_x(a):
        return lax.ppermute(a, "shard", [(s, s ^ 2) for s in range(shards)])

    def to_y(a):
        return lax.ppermute(a, "context", [(0, 1), (1, 0)])

    def after(a, *others):
        return lax.optimization_barrier((a, *others))[0]

    def turn(a, axis):
        return jnp.concatenate(
            [
                lax.dynamic_slice_in_dim(a, jnp.bitwise_xor(me, j) * chunk, chunk, axis)
                for j in range(shards)
            ],
            axis=axis,
        )

    def my_rows(a):
        return lax.dynamic_slice_in_dim(a, mine * rows, rows, 0)

    def scatter_rows(a):
        return lax.psum_scatter(a, "tensor", scatter_dimension=0, tiled=True)

    def gather_rows(a):
        return lax.all_gather(a, "tensor", axis=0, tiled=True)

    qkv_own = jnp.concatenate([w_query, w_key, w_value], axis=1)
    qkv_x = to_x(qkv_own)
    qkv = [qkv_own, to_core(qkv_own), qkv_x, to_core(qkv_x)]
    out_own = jnp.concatenate(
        [w_output.T, jnp.pad(w_router, ((0, 0), (0, 128 - experts)))], axis=1
    )
    out_x = to_x(after(out_own, qkv_x))
    outs = [out_own, to_core(out_own), out_x, to_core(out_x)]
    w_own = jnp.stack([w_gate, w_up, w_down.transpose(0, 2, 1)])
    w_core = to_core(w_own)
    groups = experts // GROUP
    half = GROUP // 2
    fetched, orders = [], []
    gate_on = out_x
    for n in range(groups):
        if pair:
            start = n * GROUP + here * half
            piece = lax.dynamic_slice_in_dim(w_own, start, half, 1)
            x_near = to_x(after(piece, gate_on))
            y_near = to_y(x_near)
            order = n * GROUP + jnp.array(
                [jnp.bitwise_xor(here, i // half) * half + i % half for i in range(GROUP)]
            )
        else:
            both = to_x(after(w_own[:, n * GROUP : (n + 1) * GROUP], gate_on))
            x_near, y_near = both[:, :half], both[:, half:]
            order = n * GROUP + jnp.arange(GROUP)
        fetched.append((x_near, y_near, to_core(x_near), to_core(y_near)))
        orders.append(order.astype(jnp.int32))
        gate_on = x_near

    x_low = turn(hidden.reshape(tokens, width), 1)
    g_low = turn(out_grad.reshape(tokens, width), 1)
    gain1, gain2 = turn(norm1_gain, 0), turn(norm2_gain, 0)
    positions = here * tokens + jnp.arange(tokens, dtype=jnp.int32)
    valid = (positions < seq_lengths[0]).astype(f32)[:, None]
    x_all = x_low.astype(f32)
    rate1 = lax.rsqrt(jnp.mean(x_all * x_all, axis=-1, keepdims=True) + EPSILON)
    h1 = (x_all * rate1 * gain1).astype(bf16)
    w_qkv = jnp.concatenate(qkv, axis=0)
    proj = nn(h1, w_qkv)
    query, key, value = proj[:, :cols], proj[:, cols : 2 * cols], proj[:, 2 * cols :]
    squares = lax.psum(
        jnp.stack([jnp.sum(query * query, axis=-1), jnp.sum(key * key, axis=-1)]), "tensor"
    )
    rate_q, rate_k = lax.rsqrt(squares / width + EPSILON)[:, :, None]
    inv_freq = 10000.0 ** (-(2.0 * jnp.arange(HEAD_DIM // 2, dtype=f32)) / HEAD_DIM)
    angles = positions.astype(f32)[:, None] * inv_freq[None, :]
    cosine, sine = jnp.cos(angles)[:, None, :], jnp.sin(angles)[:, None, :]
    split = (tokens, heads, HEAD_DIM)
    q_rot = rotate((query * rate_q * query_gain).reshape(split), cosine, sine).astype(bf16)
    k_rot = rotate((key * rate_k * key_gain).reshape(split), cosine, sine).astype(bf16)
    v_low = value.astype(bf16)
    kv = jnp.concatenate([k_rot.reshape(tokens, cols), v_low], axis=1)
    if pair:
        kv_all = jnp.concatenate([kv, to_y(kv)], axis=0)
        key_pos = jnp.concatenate([positions, (1 - here) * tokens + jnp.arange(tokens)])
    else:
        kv_all = lax.all_gather(kv, "context", axis=0, tiled=True)
        key_pos = jnp.arange(tokens * contexts)
    keys = kv_all[:, :cols].reshape(-1, heads, HEAD_DIM)
    values = kv_all[:, cols:].reshape(-1, heads, HEAD_DIM)
    causal = key_pos[None, :] <= positions[:, None]
    scores = jnp.where(
        causal[None],
        jnp.einsum("qhc,khc->hqk", q_rot, keys, preferred_element_type=f32) * scale,
        -1e30,
    )
    top = jnp.max(scores, axis=-1, keepdims=True)
    expo = jnp.exp(scores - top)
    total = jnp.sum(expo, axis=-1, keepdims=True)
    log_total = top + jnp.log(total)
    mixed = (
        jnp.einsum("hqk,khc->qhc", (expo / total).astype(bf16), values, preferred_element_type=f32)
        .astype(bf16)
        .reshape(tokens, cols)
    )
    w_out = jnp.concatenate([o[:, :cols] for o in outs], axis=0)
    w_rout = jnp.concatenate([o[:, cols : cols + experts] for o in outs], axis=0)
    attn = scatter_rows(nt(mixed, w_out).astype(bf16))

    x_part = my_rows(x_low).astype(f32)
    y1 = x_part + attn.astype(f32)
    rate2 = lax.rsqrt(jnp.mean(y1 * y1, axis=-1, keepdims=True) + EPSILON)
    h2 = gather_rows((y1 * rate2 * gain2).astype(bf16))

    logits = nn(h2, w_rout)
    expo_logit = jnp.exp(logits - jnp.max(logits, axis=-1, keepdims=True))
    router = expo_logit / jnp.sum(expo_logit, axis=-1, keepdims=True)
    routes = expert_routes.reshape(tokens, expert_routes.shape[-1])
    member = jnp.any(
        routes[:, :, None] == jnp.arange(experts, dtype=jnp.int32)[None, None, :], axis=1
    ).astype(f32)
    coef = router * member
    g_all = (g_low.astype(f32) * valid).astype(bf16)
    g_part = my_rows(g_all).astype(f32)
    h2_t, g_t = h2.T, g_all.T

    sums = None
    expert_sums = []
    for n in range(groups):
        *sums, keep, send = moe_call(
            n * GROUP, orders[n], h2, h2_t, g_all, g_t, coef, w_own, w_core, fetched[n], sums
        )
        near = (keep.astype(f32) + to_core(send).astype(f32)).astype(bf16)
        owned = (near[:, :, 0].astype(f32) + to_x(near[:, :, 1]).astype(f32)).astype(bf16)
        if pair:
            expert_sums.append(owned.astype(f32) + to_y(owned).astype(f32))
        else:
            expert_sums.append(lax.psum(owned.astype(f32), "context"))
    moe, dh, dcoef = sums
    grad_gate, grad_up = (jnp.concatenate([s[i] for s in expert_sums], axis=0) for i in (0, 1))
    grad_down = jnp.concatenate([s[2] for s in expert_sums], axis=0).transpose(0, 2, 1)

    dprob = dcoef * member
    dlog = (router * (dprob - jnp.sum(router * dprob, axis=-1, keepdims=True))).astype(bf16)
    grad_router = tn(h2, dlog)
    dh2 = scatter_rows((dh + nt(dlog, w_rout)).astype(bf16)).astype(f32)
    gain2_grad = jnp.sum(dh2 * (y1 * rate2), axis=0)
    e2 = dh2 * gain2
    dy1 = g_part + rate2 * e2 - y1 * rate2**3 * jnp.mean(e2 * y1, axis=-1, keepdims=True)
    da = gather_rows(dy1.astype(bf16))

    def chunks_to_owner(grad):
        near = (grad[0::2].astype(f32) + to_core(grad[1::2]).astype(f32)).astype(bf16)
        owned = (near[0].astype(f32) + to_x(near[1]).astype(f32)).astype(bf16)
        if pair:
            return owned.astype(f32) + to_y(owned).astype(f32)
        return lax.psum(owned.astype(f32), "context")

    sum_out = chunks_to_owner(tn(da, mixed).astype(bf16).reshape(shards, chunk, cols))

    dmixed = nn(da, w_out).astype(bf16).reshape(split)
    scores = jnp.where(
        causal[None],
        jnp.einsum("qhc,khc->hqk", q_rot, keys, preferred_element_type=f32) * scale,
        -1e30,
    )
    probs = jnp.exp(scores - log_total)
    dprobs = jnp.einsum("qhc,khc->hqk", dmixed, values, preferred_element_type=f32)
    dscores = (probs * (dprobs - jnp.sum(probs * dprobs, axis=-1, keepdims=True))).astype(bf16)
    dqr = jnp.einsum("hqk,khc->qhc", dscores, keys, preferred_element_type=f32) * scale
    dkr = jnp.einsum("hqk,qhc->khc", dscores, q_rot, preferred_element_type=f32) * scale
    dvb = jnp.einsum("hqk,qhc->khc", probs.astype(bf16), dmixed, preferred_element_type=f32)
    dkv = jnp.concatenate([dkr.reshape(-1, cols), dvb.reshape(-1, cols)], axis=1)
    if pair:
        dkv = dkv[:tokens] + to_y(dkv[tokens:].astype(bf16)).astype(f32)
    else:
        dkv = lax.psum_scatter(dkv, "context", scatter_dimension=0, tiled=True)
    dq_norm = unrotate(dqr, cosine, sine).reshape(tokens, cols)
    dk_norm = unrotate(dkv[:, :cols].reshape(split), cosine, sine).reshape(tokens, cols)
    gain_q_grad = jnp.sum(dq_norm * query * rate_q, axis=0)
    gain_k_grad = jnp.sum(dk_norm * key * rate_k, axis=0)
    eq, ek = dq_norm * query_gain, dk_norm * key_gain
    stat_q, stat_k = (
        lax.psum(jnp.stack([jnp.sum(eq * query, axis=-1), jnp.sum(ek * key, axis=-1)]), "tensor")
        / width
    )[:, :, None]
    dq = (rate_q * eq - query * rate_q**3 * stat_q).astype(bf16)
    dk = (rate_k * ek - key * rate_k**3 * stat_k).astype(bf16)
    dqkv = jnp.concatenate([dq, dk, dkv[:, cols:].astype(bf16)], axis=1)
    sum_qkv = chunks_to_owner(tn(h1, dqkv).astype(bf16).reshape(shards, chunk, 3 * cols))

    dh1 = scatter_rows(nt(dqkv, w_qkv).astype(bf16)).astype(f32)
    r1 = my_rows(rate1)
    gain1_grad = jnp.sum(dh1 * (x_part * r1), axis=0)
    e1 = dh1 * gain1
    dx = dy1 + r1 * e1 - x_part * r1**3 * jnp.mean(e1 * x_part, axis=-1, keepdims=True)
    input_grad = turn(gather_rows(dx.astype(bf16)), 1).reshape(hidden.shape)
    block = my_rows(valid) * (y1 + scatter_rows(moe.astype(bf16)).astype(f32))
    block_out = turn(gather_rows(block.astype(bf16)), 1).reshape(hidden.shape)

    gains_qk = jnp.stack([gain_q_grad, gain_k_grad])
    slot = (jnp.arange(tensors) == mine).astype(f32)[:, None, None]
    small = lax.psum(
        jnp.concatenate(
            [
                turn(gain1_grad, 0),
                turn(gain2_grad, 0),
                (slot * gains_qk[None]).reshape(-1),
                turn(grad_router, 0).T.reshape(-1),
            ]
        ),
        ("shard", "context", "tensor"),
    )
    sum_gains = lax.dynamic_slice_in_dim(
        small[2 * width : 2 * width + tensors * 2 * cols].reshape(tensors, 2, cols), mine, 1, 0
    )[0]
    sum_router = lax.dynamic_slice_in_dim(
        small[2 * width + tensors * 2 * cols :].reshape(experts, width), me * chunk, chunk, 1
    ).T
    return (
        block_out,
        input_grad,
        small[:width],
        sum_qkv[:, :cols],
        sum_qkv[:, cols : 2 * cols],
        sum_qkv[:, 2 * cols :],
        sum_gains[0],
        sum_gains[1],
        sum_out.T,
        small[width : 2 * width],
        sum_router,
        grad_gate,
        grad_up,
        grad_down,
    )


def solution(mesh):
    in_specs = (
        P("shard", "context", None),
        P(),
        P("shard", "tensor"),
        P("shard", "tensor"),
        P("shard", "tensor"),
        P("tensor"),
        P("tensor"),
        P("tensor", "shard"),
        P(),
        P("shard", None),
        P(None, "shard", "tensor"),
        P(None, "shard", "tensor"),
        P(None, "tensor", "shard"),
        P("shard"),
        P("shard", "context", None),
        P("shard", "context", None),
    )
    out_specs = (
        P("shard", "context", None),
        P("shard", "context", None),
        P(),
        P("shard", "tensor"),
        P("shard", "tensor"),
        P("shard", "tensor"),
        P("tensor"),
        P("tensor"),
        P("tensor", "shard"),
        P(),
        P("shard", None),
        P(None, "shard", "tensor"),
        P(None, "shard", "tensor"),
        P(None, "tensor", "shard"),
    )
    return jax.shard_map(body, mesh=mesh, in_specs=in_specs, out_specs=out_specs, check_vma=False)
```

```python
import functools

import jax
import jax.numpy as jnp
from jax import lax
from jax.experimental import pallas as pl
from jax.experimental.pallas import tpu as pltpu
from jax.sharding import PartitionSpec as P


HEAD_DIM = 128
EPSILON = 1e-05
GROUP = 4
f32 = jnp.float32
bf16 = jnp.bfloat16


def nn(a, b):
    return lax.dot_general(a, b, (((1,), (0,)), ((), ())), preferred_element_type=f32)


def nt(a, b):
    return lax.dot_general(a, b, (((1,), (1,)), ((), ())), preferred_element_type=f32)


def tn(a, b):
    return lax.dot_general(a, b, (((0,), (0,)), ((), ())), preferred_element_type=f32)


def moe_kernel(
    first, partial, final, base, count,
    h_ref, g_ref, coef_ref, w_own, w_core, w_x, w_xc, *refs,
):
    refs = list(refs)
    sums_in = [] if first else [refs.pop(0) for _ in range(3)]
    grads_in = refs.pop(0) if partial else None
    moe_ref, dh_ref, dc_ref = (refs.pop(0) for _ in range(3))
    outs = [refs.pop(0) for _ in range(2 if final else 1)]
    wbuf, wsems, *swap = refs
    step = pl.program_id(0)
    chunk = h_ref.shape[1] // 4
    slot = lax.rem(step, 2)
    before = 1 - slot

    def fetch(at, slot, act):
        for piece, src in enumerate((w_own.at[:, base + at], w_core.at[:, base + at], w_x.at[:, at], w_xc.at[:, at])):
            dst = wbuf.at[slot, :, pl.ds(piece * chunk, chunk)]
            act(pltpu.make_async_copy(src, dst, wsems.at[slot, piece]))

    if final:
        keep, send, got, send_sems, got_sems, free = swap
        me = lax.axis_index("shard")
        partner = {"shard": me + 1 - 2 * lax.rem(me, 2)}

        def swap_copy(slot):
            return pltpu.make_async_remote_copy(
                src_ref=send.at[slot],
                dst_ref=got.at[slot],
                send_sem=send_sems.at[slot],
                recv_sem=got_sems.at[slot],
                device_id=partner,
                device_id_type=pl.DeviceIdType.MESH,
            )

    @pl.when(step == 0)
    def _():
        fetch(0, 0, lambda c: c.start())
        if final:
            barrier = pltpu.get_barrier_semaphore()
            pl.semaphore_signal(
                barrier, inc=1, device_id=partner, device_id_type=pl.DeviceIdType.MESH
            )
            pl.semaphore_wait(barrier, 1)
        for i, ref in enumerate((moe_ref, dh_ref, dc_ref)):
            ref[...] = jnp.zeros_like(ref) if first else sums_in[i][...]

    @pl.when(step + 1 < count)
    def _():
        fetch(step + 1, before, lambda c: c.start())

    @pl.when(step < count)
    def _():
        fetch(step, slot, lambda c: c.wait())
        lanes = lax.broadcasted_iota(jnp.int32, coef_ref.shape, 1)
        picked = lanes == base + step
        coef = jnp.sum(jnp.where(picked, coef_ref[...], 0.0), axis=1, keepdims=True)
        wg, wu, wd = wbuf.at[slot, 0], wbuf.at[slot, 1], wbuf.at[slot, 2]
        gate = nn(h_ref[...], wg[...])
        up = nn(h_ref[...], wu[...])
        dz_plain = nn(g_ref[...], wd[...])
        sig = jax.nn.sigmoid(gate)
        act = gate * sig
        z = act * up
        z_coef = (z * coef).astype(bf16)
        dcoef = jnp.sum(z * dz_plain, axis=1, keepdims=True)
        dc_ref[...] += jnp.where(picked, dcoef, 0.0)
        dz = dz_plain * coef
        dgate = (dz * up * (sig * (1.0 + gate * (1.0 - sig)))).astype(bf16)
        dup = (dz * act).astype(bf16)
        for j in range(4):
            rows = slice(j * chunk, (j + 1) * chunk)
            moe_ref[:, rows] += nt(z_coef, wd[rows, :])
            dh_ref[:, rows] += nt(dgate, wg[rows, :]) + nt(dup, wu[rows, :])
            for i, (left, right) in enumerate(((dgate, h_ref), (dup, h_ref), (z_coef, g_ref))):
                grad = tn(left, right[:, rows])
                if partial:
                    grad = grad + grads_in[j, i, 0].astype(f32)
                if final:
                    (send if j % 2 else keep)[slot, j // 2, i] = grad.astype(bf16)
                else:
                    outs[0][j, i, 0] = grad.astype(bf16)
        if final:

            @pl.when(step >= 2)
            def _():
                pl.semaphore_wait(free, 1)

            swap_copy(slot).start()

    if final:

        @pl.when(step >= 1)
        def _():
            swap_copy(before).wait()
            for j in range(2):
                outs[j][:, 0] = (
                    keep[before, j].astype(f32) + got[before, j].astype(f32)
                ).astype(bf16)

            @pl.when(step <= count - 2)
            def _():
                pl.semaphore_signal(
                    free, inc=1, device_id=partner, device_id_type=pl.DeviceIdType.MESH
                )


def moe_call(ident, base, h, g, coef, weights, sums, grads, final):
    tokens, width = h.shape
    hidden = weights[0].shape[3]
    chunk = width // 4
    first, partial = sums is None, grads is not None

    def whole(shape):
        return pl.BlockSpec(shape, lambda i: (0,) * len(shape), pipeline_mode=pl.Buffered(1))

    def expert_block(lead):
        at = (lambda i: jnp.minimum(i, GROUP - 1)) if lead else (lambda i: jnp.maximum(i - 1, 0))
        shape = (*lead, 3, 1, hidden, chunk)
        return pl.BlockSpec(shape, lambda i: (0,) * len(lead) + (0, at(i), 0, 0))

    totals = [jax.ShapeDtypeStruct(a.shape, f32) for a in (h, h, coef)]
    scratch = [pltpu.VMEM((2, 3, width, hidden), bf16), pltpu.SemaphoreType.DMA((2, 4))]
    if final:
        scratch += [pltpu.VMEM((2, 2, 3, hidden, chunk), bf16)] * 3
        scratch += [pltpu.SemaphoreType.DMA((2,))] * 2 + [pltpu.SemaphoreType.REGULAR]
    lead = () if final else (4,)
    grad_shape = jax.ShapeDtypeStruct((*lead, 3, GROUP, hidden, chunk), bf16)
    extra = ({} if not final else {"collective_id": ident, "has_side_effects": True})
    return pl.pallas_call(
        functools.partial(moe_kernel, first, partial, final, base, GROUP),
        grid=(GROUP + 1 if final else GROUP,),
        in_specs=[whole(a.shape) for a in (h, g, coef)]
        + [pl.BlockSpec(memory_space=pl.ANY)] * 4
        + ([] if first else [whole(a.shape) for a in sums])
        + ([expert_block((4,))] if partial else []),
        out_specs=[whole(a.shape) for a in totals] + [expert_block(lead)] * (2 if final else 1),
        scratch_shapes=scratch,
        out_shape=totals + [grad_shape] * (2 if final else 1),
        compiler_params=pltpu.CompilerParams(
            dimension_semantics=("arbitrary",), vmem_limit_bytes=60 * 1024 * 1024, **extra
        ),
        cost_estimate=pl.CostEstimate(
            flops=18 * tokens * width * hidden * GROUP,
            bytes_accessed=12 * width * hidden * GROUP + 32 * tokens * width,
            transcendentals=GROUP * tokens * hidden,
        ),
    )(h, g, coef, *weights, *(() if first else sums), *((grads,) if partial else ()))


def finish_kernel(count, more, places, own_ref, *refs):
    gate_ref, up_ref, down_ref = refs[-3:]

    def put(ref):
        gate_ref[0] = ref[0, 0].astype(f32).T
        up_ref[0] = ref[1, 0].astype(f32).T
        down_ref[0] = ref[2, 0].astype(f32)

    pl.when(pl.program_id(0) < count)(lambda: put(own_ref))
    if more:
        pl.when(pl.program_id(0) >= count)(lambda: put(refs[0]))


def finish_call(places, experts, own, other, grads):
    count, hidden, chunk = own.shape[1:]
    first = grads is None
    shapes = [(experts, chunk, hidden), (experts, chunk, hidden), (experts, hidden, chunk)]
    pieces = [pl.BlockSpec((3, 1, hidden, chunk), lambda i, p: (0, jnp.minimum(i, count - 1), 0, 0))]
    if other is not None:
        pieces.append(
            pl.BlockSpec((3, 1, hidden, chunk), lambda i, p: (0, jnp.maximum(i - count, 0), 0, 0))
        )
    old = 1 + len(pieces)
    return pl.pallas_call(
        functools.partial(finish_kernel, count, other is not None),
        grid_spec=pltpu.PrefetchScalarGridSpec(
            num_scalar_prefetch=1,
            grid=(count * len(pieces),),
            in_specs=pieces + ([] if first else [pl.BlockSpec(memory_space=pl.ANY)] * 3),
            out_specs=[pl.BlockSpec((1, *s[1:]), lambda i, p: (p[i], 0, 0)) for s in shapes],
        ),
        out_shape=[jax.ShapeDtypeStruct(s, f32) for s in shapes],
        input_output_aliases={} if first else {old: 0, old + 1: 1, old + 2: 2},
        compiler_params=pltpu.CompilerParams(
            dimension_semantics=("arbitrary",), vmem_limit_bytes=24 * 1024 * 1024
        ),
        cost_estimate=pl.CostEstimate(
            flops=0, bytes_accessed=36 * count * chunk * hidden, transcendentals=0
        ),
        name="finish",
    )(places, own, *(() if other is None else (other,)), *(() if first else grads))


def qkv_kernel(x_ref, gain_ref, w0, w1, w2, w3, proj_ref, h_ref, rate_ref, sq_ref, sq_acc):
    step = pl.program_id(0)

    @pl.when(step == 0)
    def _():
        x = x_ref[...].astype(f32)
        rate = lax.rsqrt(jnp.mean(x * x, axis=-1, keepdims=True) + EPSILON)
        rate_ref[...] = rate
        h_ref[...] = (x * rate * gain_ref[...]).astype(bf16)
        sq_acc[...] = jnp.zeros_like(sq_acc)

    chunk = w0.shape[0]
    proj = sum(nn(h_ref[:, j * chunk : (j + 1) * chunk], w[...]) for j, w in enumerate((w0, w1, w2, w3)))
    proj_ref[...] = proj
    lanes = lax.broadcasted_iota(jnp.int32, sq_acc.shape, 1)
    sq_acc[...] += jnp.where(lanes == step, jnp.sum(proj * proj, axis=-1, keepdims=True), 0.0)

    @pl.when(step == 2)
    def _():
        sq_ref[...] = sq_acc[...].T[: sq_ref.shape[0]]


def qkv_call(x, gain, weights):
    tokens, width = x.shape
    chunk, cols = weights[0].shape[0], weights[0].shape[1] // 3
    return pl.pallas_call(
        qkv_kernel,
        grid=(3,),
        in_specs=[
            pl.BlockSpec((tokens, width), lambda i: (0, 0), pipeline_mode=pl.Buffered(1)),
            pl.BlockSpec((1, width), lambda i: (0, 0)),
        ]
        + [pl.BlockSpec((chunk, cols), lambda i: (0, i))] * 4,
        out_specs=[
            pl.BlockSpec((tokens, cols), lambda i: (0, i)),
            pl.BlockSpec((tokens, width), lambda i: (0, 0)),
            pl.BlockSpec((tokens, 1), lambda i: (0, 0)),
            pl.BlockSpec((8, tokens), lambda i: (0, 0)),
        ],
        scratch_shapes=[pltpu.VMEM((tokens, 128), f32)],
        out_shape=[
            jax.ShapeDtypeStruct((tokens, 3 * cols), f32),
            jax.ShapeDtypeStruct((tokens, width), bf16),
            jax.ShapeDtypeStruct((tokens, 1), f32),
            jax.ShapeDtypeStruct((8, tokens), f32),
        ],
        compiler_params=pltpu.CompilerParams(
            dimension_semantics=("arbitrary",), vmem_limit_bytes=40 * 1024 * 1024
        ),
        cost_estimate=pl.CostEstimate(
            flops=6 * tokens * width * cols, bytes_accessed=12 * width * cols, transcendentals=tokens
        ),
        name="qkv",
    )(x, gain[None], *weights)


def meet(peers):
    barrier = pltpu.get_barrier_semaphore()
    for here, place in peers:

        @pl.when(here)
        def _(place=place):
            pl.semaphore_signal(
                barrier, inc=1, device_id={"tensor": place}, device_id_type=pl.DeviceIdType.MESH
            )

    pl.semaphore_wait(barrier, sum(here.astype(jnp.int32) for here, _ in peers))


def line_kernel(n, subs, streams, *refs):
    refs = list(refs)
    ins = [[refs.pop(0) for _ in range(1 + extra)] for _, extra, _ in streams]
    outs = [[refs.pop(0) for _ in range(1 + more)] for _, _, more in streams]
    scratch = [[refs.pop(0) for _ in range(3)] for _ in streams]
    z = lax.axis_index("tensor")
    inner = (z > 0, z < n - 1)
    side = (z - 1, z + 1)
    meet([(inner[0], z - 1), (inner[1], z + 1)])

    class Stream:
        def __init__(self, finish, part_ref, extras, out_ref, more, buf, total, sems):
            self.finish, self.part, self.extras, self.out = finish, part_ref, extras, out_ref
            self.more, self.buf, self.total, self.sems = more, buf, total, sems
            self.block = part_ref.shape[0] // n
            self.size = self.block // subs

        def rows(self, b, s):
            return pl.ds(pl.multiple_of(b * self.block + s * self.size, self.size), self.size)

        def copy(self, kind, way, b, s):
            at = self.rows(b, s)
            return pltpu.make_async_remote_copy(
                src_ref=self.out.at[at] if kind else self.buf.at[way, 0, at],
                dst_ref=self.out.at[at] if kind else self.buf.at[way, 1, at],
                send_sem=self.sems.at[2 * kind, way, b, s],
                recv_sem=self.sems.at[2 * kind + 1, way, b, s],
                device_id={"tensor": side[way]},
                device_id_type=pl.DeviceIdType.MESH,
            )

        def open(self, way):
            @pl.when(jnp.logical_not(inner[1 - way]))
            def _():
                for s in range(subs):
                    for i in range(1, n):
                        b = n - i if way else i - 1
                        self.buf[way, 0, self.rows(b, s)] = self.part[self.rows(b, s)]
                        self.copy(0, way, b, s).start()

        def pass_on(self, way, b, s):
            @pl.when(inner[1 - way] & ((z < b) if way else (z > b)))
            def _():
                at = self.rows(b, s)
                self.copy(0, way, b, s).wait_recv()
                mine = self.part[at].astype(f32)
                self.buf[way, 0, at] = (mine + self.buf[way, 1, at].astype(f32)).astype(bf16)
                self.copy(0, way, b, s).start()

        def own(self, s):
            at = self.rows(z, s)
            self.total[...] = self.part[at].astype(f32)
            for way in (0, 1):

                @pl.when(inner[1 - way])
                def _(way=way):
                    self.copy(0, way, z, s).wait_recv()
                    self.total[...] += self.buf[way, 1, at].astype(f32)

            local = pl.ds(s * self.size, self.size)
            self.out[at] = self.finish(s, self.total[...], at, local, self.extras, self.more)
            for way in (0, 1):

                @pl.when(inner[way])
                def _(way=way):
                    self.copy(1, way, z, s).start()

        def forward(self, d, s):
            for way in (0, 1):
                b = z - d if way else z + d

                @pl.when(inner[way] & ((b >= 0) if way else (b <= n - 1)))
                def _(way=way, b=b):
                    self.copy(1, way, b, s).wait_recv()
                    self.copy(1, way, b, s).start()

        def close(self, way, b, s):
            ahead = (z < b) if way else (z > b)
            past = (z > b) if way else (z < b)

            @pl.when(past & jnp.logical_not(inner[way]))
            def _():
                self.copy(1, way, b, s).wait_recv()

            @pl.when(ahead)
            def _():
                self.copy(0, way, b, s).wait_send()

            @pl.when(inner[way] & jnp.logical_not(ahead))
            def _():
                self.copy(1, way, b, s).wait_send()

    flows = [
        Stream(finish, i[0], i[1:], o[0], o[1:], *c)
        for (finish, _, _), i, o, c in zip(streams, ins, outs, scratch)
    ]
    for flow in flows:
        for way in (0, 1):
            flow.open(way)
    for s in range(subs + 1):
        for flow in flows:
            if s < subs:
                for i in range(1, n):
                    flow.pass_on(1, n - i, s)
                    flow.pass_on(0, i - 1, s)
            if s:
                flow.own(s - 1)
                for d in range(1, n - 1):
                    if s - 1 >= d:
                        flow.forward(d, s - 1 - d)
    for s in range(subs):
        for flow in flows:
            for d in range(1, n - 1):
                if s + d >= subs:
                    flow.forward(d, s)
    for flow in flows:
        for s in range(subs):
            for b in range(n):
                for way in (0, 1):
                    flow.close(way, b, s)


def line_call(ident, n, streams):
    subs = 2
    vmem = pl.BlockSpec(memory_space=pltpu.VMEM)
    shapes, scratch, inputs, kinds = [], [], [], []
    for finish, part, extras, more in streams:
        tokens, width = part.shape
        kinds.append((finish, len(extras), len(more)))
        inputs += [part, *extras]
        shapes += [jax.ShapeDtypeStruct((tokens, width), bf16)]
        shapes += [jax.ShapeDtypeStruct(m, f32) for m in more]
        scratch += [
            pltpu.VMEM((2, 2, tokens, width), bf16),
            pltpu.VMEM((tokens // n // subs, width), f32),
            pltpu.SemaphoreType.DMA((4, 2, n, subs)),
        ]
    return pl.pallas_call(
        functools.partial(line_kernel, n, subs, kinds),
        in_specs=[vmem] * len(inputs),
        out_specs=[vmem] * len(shapes),
        out_shape=shapes,
        scratch_shapes=scratch,
        compiler_params=pltpu.CompilerParams(
            collective_id=ident, has_side_effects=True, vmem_limit_bytes=58 * 1024 * 1024
        ),
        cost_estimate=pl.CostEstimate(
            flops=12000 * tokens * width, bytes_accessed=8 * tokens * width, transcendentals=0
        ),
    )(*inputs)


def after_attention(s, total, whole, local, refs, more):
    x_ref, gain_ref = refs
    y_ref, rate_ref = more
    y = x_ref[whole].astype(f32) + total
    rate = lax.rsqrt(jnp.mean(y * y, axis=-1, keepdims=True) + EPSILON)
    y_ref[local] = y
    rate_ref[local] = rate
    return (y * rate * gain_ref[...]).astype(bf16)


def norm_back(total, base, x, rate, gain_ref, grad_ref, s):
    terms = jnp.sum(total * (x * rate), axis=0, keepdims=True)
    grad_ref[...] = terms if s == 0 else grad_ref[...] + terms
    e = total * gain_ref[...]
    return base + rate * e - x * (rate * rate * rate) * jnp.mean(e * x, axis=-1, keepdims=True)


def after_experts(s, total, whole, local, refs, more):
    g_ref, y_ref, rate_ref, gain_ref = refs
    dy_ref, grad_ref = more
    dy = norm_back(
        total, g_ref[whole].astype(f32), y_ref[local], rate_ref[local], gain_ref, grad_ref, s
    )
    dy_ref[local] = dy
    return dy.astype(bf16)


def after_projections(s, total, whole, local, refs, more):
    x_ref, dy_ref, rate_ref, gain_ref = refs
    (grad_ref,) = more
    x = x_ref[whole].astype(f32)
    dx = norm_back(total, dy_ref[local], x, rate_ref[whole], gain_ref, grad_ref, s)
    return dx.astype(bf16)


def block_rows(s, total, whole, local, refs, more):
    y_ref, valid_ref = refs
    return (valid_ref[whole] * (y_ref[local] + total)).astype(bf16)


def exchange(n, mine_ref, got_ref, sems):
    z = lax.axis_index("tensor")
    places = [lax.rem(z + d, n) for d in range(n)]
    meet([(z >= 0, p) for p in places[1:]])
    copies = [
        pltpu.make_async_remote_copy(
            src_ref=mine_ref,
            dst_ref=got_ref.at[z],
            send_sem=sems.at[0, d],
            recv_sem=sems.at[1, d],
            device_id={"tensor": places[d]},
            device_id_type=pl.DeviceIdType.MESH,
        )
        for d in range(1, n)
    ]
    for c in copies:
        c.start()
    got_ref[z] = mine_ref[...]

    def total():
        for c in copies:
            c.wait()
        return sum(got_ref[i] for i in range(n))

    return total


def rope_kernel(n, proj_ref, sq_ref, gq_ref, gk_ref, cos_ref, sin_ref, q_ref, kv_ref, rate_ref, mine, got, sems):
    _, cols = q_ref.shape
    mine[...] = sq_ref[...]
    total = exchange(n, mine, got, sems)
    kv_ref[:, cols:] = proj_ref[:, 2 * cols :].astype(bf16)
    sums = total()
    rates = lax.rsqrt(sums / (n * cols) + EPSILON).T
    rate_ref[...] = rates
    cosine, sine = cos_ref[...], sin_ref[...]

    def turned(part, rate, gain, head):
        at = slice(head * HEAD_DIM, (head + 1) * HEAD_DIM)
        a = proj_ref[:, part * cols + head * HEAD_DIM : part * cols + (head + 1) * HEAD_DIM]
        a = a * rate * gain[:, at]
        return (a * cosine + pltpu.roll(a, HEAD_DIM // 2, 1) * sine).astype(bf16)

    for head in range(cols // HEAD_DIM):
        at = slice(head * HEAD_DIM, (head + 1) * HEAD_DIM)
        q_ref[:, at] = turned(0, rates[:, 0:1], gq_ref, head)
        kv_ref[:, at] = turned(1, rates[:, 1:2], gk_ref, head)


def exchange_scratch(n, tokens, rows=8):
    return [
        pltpu.VMEM((rows, tokens), f32),
        pltpu.VMEM((n, rows, tokens), f32),
        pltpu.SemaphoreType.DMA((2, n)),
    ]


def rope_call(n, proj, sq, gq, gk, cosine, sine):
    tokens, cols = proj.shape[0], proj.shape[1] // 3
    vmem = pl.BlockSpec(memory_space=pltpu.VMEM)
    return pl.pallas_call(
        functools.partial(rope_kernel, n),
        in_specs=[vmem] * 6,
        out_specs=[vmem] * 3,
        out_shape=[
            jax.ShapeDtypeStruct((tokens, cols), bf16),
            jax.ShapeDtypeStruct((tokens, 2 * cols), bf16),
            jax.ShapeDtypeStruct((tokens, 8), f32),
        ],
        scratch_shapes=exchange_scratch(n, tokens),
        compiler_params=pltpu.CompilerParams(
            collective_id=1, has_side_effects=True, vmem_limit_bytes=40 * 1024 * 1024
        ),
        cost_estimate=pl.CostEstimate(
            flops=2000 * tokens * cols, bytes_accessed=18 * tokens * cols, transcendentals=tokens
        ),
        name="rope",
    )(proj, sq, gq[None], gk[None], cosine, sine)


def qk_back_kernel(
    n, dq_ref, dk_ref, dv_ref, far_ref, proj_ref, rate_ref, gq_ref, gk_ref, cos_ref, sin_ref, dc_ref,
    out_ref, grad_ref, dcs_ref, dn, mine, got, sems,
):
    tokens, cols = dq_ref.shape
    cosine, sine = cos_ref[...], sin_ref[...]
    lanes = lax.broadcasted_iota(jnp.int32, (tokens, HEAD_DIM), 1)
    stats = jnp.zeros((tokens, HEAD_DIM), f32)
    rates = rate_ref[...]
    for part, gain in ((0, gq_ref), (1, gk_ref)):
        stat = jnp.zeros((tokens, 1), f32)
        rate = rates[:, part : part + 1]
        for head in range(cols // HEAD_DIM):
            at = slice(head * HEAD_DIM, (head + 1) * HEAD_DIM)
            if part:
                a = dk_ref[:, at] + far_ref[:, at].astype(f32)
            else:
                a = dq_ref[:, at]
            a = a * cosine - pltpu.roll(a, HEAD_DIM // 2, 1) * sine
            plain = proj_ref[:, part * cols + head * HEAD_DIM : part * cols + (head + 1) * HEAD_DIM]
            grad_ref[part : part + 1, at] = jnp.sum(a * plain * rate, axis=0, keepdims=True)
            a = a * gain[:, at]
            dn[part, :, at] = a
            stat += jnp.sum(a * plain, axis=-1, keepdims=True)
        stats = jnp.where(lanes == part, stat, stats)
    mine[:8] = stats.T[:8]
    mine[8:] = dc_ref[...]
    total = exchange(n, mine, got, sems)
    out_ref[:, 2 * cols :] = (dv_ref[...] + far_ref[:, cols:].astype(f32)).astype(bf16)
    whole = total()
    dcs_ref[...] = whole[8:]
    means = (whole[:8] / (n * cols)).T
    for part in (0, 1):
        rate = rates[:, part : part + 1]
        factor = rate * rate * rate * means[:, part : part + 1]
        at = slice(part * cols, (part + 1) * cols)
        out_ref[:, at] = (rate * dn[part] - proj_ref[:, at] * factor).astype(bf16)


def qk_back_call(n, dq, dk, dv, far, proj, rates, gq, gk, cosine, sine, dcoef):
    tokens, cols = dq.shape
    vmem = pl.BlockSpec(memory_space=pltpu.VMEM)
    near = pl.BlockSpec((tokens, cols), lambda i: (0, 0))
    return pl.pallas_call(
        functools.partial(qk_back_kernel, n),
        grid=(1,),
        in_specs=[vmem, near, near] + [vmem] * 8,
        out_specs=[vmem] * 3,
        out_shape=[
            jax.ShapeDtypeStruct((tokens, 3 * cols), bf16),
            jax.ShapeDtypeStruct((8, cols), f32),
            jax.ShapeDtypeStruct(dcoef.shape, f32),
        ],
        scratch_shapes=[pltpu.VMEM((2, tokens, cols), f32)]
        + exchange_scratch(n, tokens, 8 + dcoef.shape[0]),
        compiler_params=pltpu.CompilerParams(
            collective_id=2, has_side_effects=True, vmem_limit_bytes=40 * 1024 * 1024
        ),
        cost_estimate=pl.CostEstimate(
            flops=2000 * tokens * cols, bytes_accessed=30 * tokens * cols, transcendentals=0
        ),
        name="qk_back",
    )(dq, dk, dv, far, proj, rates, gq[None], gk[None], cosine, sine, dcoef)


def gains_kernel(sizes, both, in_ref, out_ref, mine, *bufs):
    mine[...] = in_ref[...]
    peers = []
    for axis, n in sizes:
        here = lax.axis_index(axis)
        peers += [(axis, d, lax.rem(here + d, n)) for d in range(1, n)]
    barrier = pltpu.get_barrier_semaphore()
    for axis, _, place in peers:
        pl.semaphore_signal(
            barrier, inc=1, device_id={axis: place}, device_id_type=pl.DeviceIdType.MESH
        )
    pl.semaphore_wait(barrier, len(peers))
    for k, (axis, n) in enumerate(sizes):
        got, sems = bufs[2 * k : 2 * k + 2]
        here = lax.axis_index(axis)
        rows = pl.ds(0, both if axis == "tensor" else mine.shape[0])
        copies = [
            pltpu.make_async_remote_copy(
                src_ref=mine.at[rows],
                dst_ref=got.at[here],
                send_sem=sems.at[0, d],
                recv_sem=sems.at[1, d],
                device_id={axis: place},
                device_id_type=pl.DeviceIdType.MESH,
            )
            for a, d, place in peers
            if a == axis
        ]
        for c in copies:
            c.start()
        got[here] = mine[rows]
        for c in copies:
            c.wait()
        mine[rows] = sum(got[i] for i in range(n))
    out_ref[...] = mine[...]


def gains_call(sizes, both, values):
    rows = values.shape[0]
    vmem = pl.BlockSpec(memory_space=pltpu.VMEM)
    scratch = [pltpu.VMEM((rows, 128), f32)]
    for axis, n in sizes:
        scratch += [
            pltpu.VMEM((n, both if axis == "tensor" else rows, 128), f32),
            pltpu.SemaphoreType.DMA((2, n)),
        ]
    return pl.pallas_call(
        functools.partial(gains_kernel, sizes, both),
        in_specs=[vmem],
        out_specs=vmem,
        out_shape=jax.ShapeDtypeStruct(values.shape, f32),
        scratch_shapes=scratch,
        compiler_params=pltpu.CompilerParams(collective_id=6, has_side_effects=True),
        cost_estimate=pl.CostEstimate(flops=10000000, bytes_accessed=100000, transcendentals=0),
        name="gains",
    )(values)


def grads_kernel(count, *refs):
    pairs = [(refs[2 * i], refs[2 * i + 1]) for i in range(count)]
    out0, out2, send, got, send_sems, got_sems = refs[2 * count :]
    me = lax.axis_index("shard")
    partner = {"shard": me + 1 - 2 * lax.rem(me, 2)}
    chunk = send.shape[1]
    barrier = pltpu.get_barrier_semaphore()
    pl.semaphore_signal(barrier, inc=1, device_id=partner, device_id_type=pl.DeviceIdType.MESH)
    pl.semaphore_wait(barrier, 1)

    def products(j, put):
        col = 0
        for left, right in pairs:
            n = right.shape[1]
            put(slice(col, col + n), tn(left[:, j * chunk : (j + 1) * chunk], right[...]))
            col += n

    copies = []
    for k, j in enumerate((1, 3)):

        def store(at, value, k=k):
            send[k, :, at] = value.astype(bf16)

        products(j, store)
        copies.append(
            pltpu.make_async_remote_copy(
                src_ref=send.at[k],
                dst_ref=got.at[k],
                send_sem=send_sems.at[k],
                recv_sem=got_sems.at[k],
                device_id=partner,
                device_id_type=pl.DeviceIdType.MESH,
            )
        )
        copies[k].start()
    for k, (j, out) in enumerate(((0, out0), (2, out2))):
        copies[k].wait_recv()

        def store(at, value, k=k, out=out):
            out[:, at] = (value + got[k, :, at].astype(f32)).astype(bf16)

        products(j, store)
    for c in copies:
        c.wait_send()


def grads_call(ident, pairs):
    tokens, width = pairs[0][0].shape
    chunk, cols = width // 4, sum(b.shape[1] for _, b in pairs)
    vmem = pl.BlockSpec(memory_space=pltpu.VMEM)
    return pl.pallas_call(
        functools.partial(grads_kernel, len(pairs)),
        in_specs=[vmem] * (2 * len(pairs)),
        out_specs=[vmem] * 2,
        out_shape=[jax.ShapeDtypeStruct((chunk, cols), bf16)] * 2,
        scratch_shapes=[pltpu.VMEM((2, chunk, cols), bf16)] * 2 + [pltpu.SemaphoreType.DMA((2,))] * 2,
        compiler_params=pltpu.CompilerParams(
            collective_id=ident, has_side_effects=True, vmem_limit_bytes=50 * 1024 * 1024
        ),
        cost_estimate=pl.CostEstimate(
            flops=2 * tokens * width * cols, bytes_accessed=4 * tokens * width, transcendentals=0
        ),
    )(*(a for p in pairs for a in p))


def masked_scores(base, q, keys, scale, flip):
    tokens = q.shape[0]
    raw = (nt(keys, q) if flip else nt(q, keys)) * scale
    axis = 0 if flip else 1
    parts = []
    for i in range(keys.shape[0] // tokens):
        rows = slice(i * tokens, (i + 1) * tokens)
        part = raw[rows] if flip else raw[:, rows]
        key_pos = base[i + 1] + lax.broadcasted_iota(jnp.int32, part.shape, axis)
        query_pos = base[0] + lax.broadcasted_iota(jnp.int32, part.shape, 1 - axis)
        parts.append(jnp.where(key_pos <= query_pos, part, -1e30))
    return jnp.concatenate(parts, axis=axis)


def attention_kernel(scale, base, q_ref, k_ref, v_ref, w0, w1, w2, w3, mixed_ref, lse_ref, part_ref, lse_acc):
    head = pl.program_id(0)
    scores = masked_scores(base, q_ref[...], k_ref[...], scale, False)
    top = jnp.max(scores, axis=-1, keepdims=True)
    expo = jnp.exp(scores - top)
    total = jnp.sum(expo, axis=-1, keepdims=True)
    mixed = nn((expo / total).astype(bf16), v_ref[...]).astype(bf16)
    for h in range(mixed_ref.shape[1] // HEAD_DIM):

        @pl.when(head == h)
        def _(h=h):
            mixed_ref[:, h * HEAD_DIM : (h + 1) * HEAD_DIM] = mixed

    @pl.when(head == 0)
    def _():
        lse_acc[...] = jnp.zeros_like(lse_acc)

    lanes = lax.broadcasted_iota(jnp.int32, lse_acc.shape, 1)
    lse_acc[...] += jnp.where(lanes == head, top + jnp.log(total), 0.0)

    @pl.when(head == pl.num_programs(0) - 1)
    def _():
        lse_ref[...] = lse_acc[...].T[: lse_ref.shape[0]]
        chunk = w0.shape[0]
        for j, w in enumerate((w0, w1, w2, w3)):
            part_ref[:, j * chunk : (j + 1) * chunk] = nt(mixed_ref[...], w[...]).astype(bf16)


def attention_call(base, q, kv, weights, scale):
    tokens, cols = q.shape
    heads, keys, chunk = cols // HEAD_DIM, kv.shape[0], weights[0].shape[0]
    return pl.pallas_call(
        functools.partial(attention_kernel, scale),
        grid_spec=pltpu.PrefetchScalarGridSpec(
            num_scalar_prefetch=1,
            grid=(heads,),
            in_specs=[
                pl.BlockSpec((tokens, HEAD_DIM), lambda h, b: (0, h)),
                pl.BlockSpec((keys, HEAD_DIM), lambda h, b: (0, h)),
                pl.BlockSpec((keys, HEAD_DIM), lambda h, b: (0, heads + h)),
            ]
            + [pl.BlockSpec((chunk, cols), lambda h, b: (0, 0), pipeline_mode=pl.Buffered(1))] * 4,
            out_specs=[
                pl.BlockSpec((tokens, cols), lambda h, b: (0, 0)),
                pl.BlockSpec((8, tokens), lambda h, b: (0, 0)),
                pl.BlockSpec((tokens, 4 * chunk), lambda h, b: (0, 0)),
            ],
            scratch_shapes=[pltpu.VMEM((tokens, 128), f32)],
        ),
        out_shape=[
            jax.ShapeDtypeStruct((tokens, cols), bf16),
            jax.ShapeDtypeStruct((8, tokens), f32),
            jax.ShapeDtypeStruct((tokens, 4 * chunk), bf16),
        ],
        compiler_params=pltpu.CompilerParams(
            dimension_semantics=("arbitrary",), vmem_limit_bytes=50 * 1024 * 1024
        ),
        cost_estimate=pl.CostEstimate(
            flops=4 * tokens * keys * cols * 4 + 8 * tokens * cols * chunk,
            bytes_accessed=8 * tokens * cols,
            transcendentals=heads * tokens * keys,
        ),
        name="attention",
    )(base, q, kv, kv, *weights)


def attention_back_kernel(
    scale, base, da_ref, q_ref, k_ref, v_ref, lse_ref, w0, w1, w2, w3, dq_ref, dk_ref, dv_ref, dmix
):
    head = pl.program_id(0)

    @pl.when(head == 0)
    def _():
        chunk = w0.shape[0]
        whole = sum(
            nn(da_ref[:, j * chunk : (j + 1) * chunk], w[...])
            for j, w in enumerate((w0, w1, w2, w3))
        ).astype(bf16)
        for h in range(dmix.shape[0]):
            dmix[h] = whole[:, h * HEAD_DIM : (h + 1) * HEAD_DIM]

    q, keys, values, dm = q_ref[...], k_ref[...], v_ref[...], dmix[head]
    scores = masked_scores(base, q, keys, scale, True)
    probs = jnp.exp(scores - lse_ref[pl.ds(head, 1), :])
    dprobs = nt(values, dm)
    ds = (probs * (dprobs - jnp.sum(probs * dprobs, axis=0, keepdims=True))).astype(bf16)
    dq_ref[...] = tn(ds, keys) * scale
    dk_ref[...] = nn(ds, q) * scale
    dv_ref[...] = nn(probs.astype(bf16), dm)


def attention_back_call(base, da, q, kv, lse, weights, scale):
    tokens, cols = q.shape
    heads, keys, chunk = cols // HEAD_DIM, kv.shape[0], weights[0].shape[0]
    return pl.pallas_call(
        functools.partial(attention_back_kernel, scale),
        grid_spec=pltpu.PrefetchScalarGridSpec(
            num_scalar_prefetch=1,
            grid=(heads,),
            in_specs=[
                pl.BlockSpec(da.shape, lambda h, b: (0, 0), pipeline_mode=pl.Buffered(1)),
                pl.BlockSpec((tokens, HEAD_DIM), lambda h, b: (0, h)),
                pl.BlockSpec((keys, HEAD_DIM), lambda h, b: (0, h)),
                pl.BlockSpec((keys, HEAD_DIM), lambda h, b: (0, heads + h)),
                pl.BlockSpec(lse.shape, lambda h, b: (0, 0)),
            ]
            + [pl.BlockSpec((chunk, cols), lambda h, b: (0, 0), pipeline_mode=pl.Buffered(1))] * 4,
            out_specs=[
                pl.BlockSpec((tokens, HEAD_DIM), lambda h, b: (0, h)),
                pl.BlockSpec((keys, HEAD_DIM), lambda h, b: (0, h)),
                pl.BlockSpec((keys, HEAD_DIM), lambda h, b: (0, h)),
            ],
            scratch_shapes=[pltpu.VMEM((heads, tokens, HEAD_DIM), bf16)],
        ),
        out_shape=[
            jax.ShapeDtypeStruct((tokens, cols), f32),
            jax.ShapeDtypeStruct((keys, cols), f32),
            jax.ShapeDtypeStruct((keys, cols), f32),
        ],
        compiler_params=pltpu.CompilerParams(
            dimension_semantics=("arbitrary",), vmem_limit_bytes=50 * 1024 * 1024
        ),
        cost_estimate=pl.CostEstimate(
            flops=10 * tokens * keys * cols + 8 * tokens * cols * chunk,
            bytes_accessed=24 * tokens * cols,
            transcendentals=heads * tokens * keys,
        ),
        name="attention_back",
    )(base, da, q, kv, kv, lse, *weights)


def body(
    hidden, norm1_gain, w_query, w_key, w_value, query_gain, key_gain, w_output,
    norm2_gain, w_router, w_gate, w_up, w_down, seq_lengths, expert_routes, out_grad,
):
    slots, tokens, width = hidden.shape
    shards, contexts, tensors = (
        lax.axis_size("shard"),
        lax.axis_size("context"),
        lax.axis_size("tensor"),
    )
    assert slots == 1 and shards == 4
    me, here = lax.axis_index("shard"), lax.axis_index("context")
    pair = contexts == 2
    chunk = width // shards
    cols = w_query.shape[1]
    experts = w_gate.shape[0]
    scale = HEAD_DIM ** (-0.5)
    rows = tokens // tensors

    def to_core(a):
        return lax.ppermute(a, "shard", [(s, s ^ 1) for s in range(shards)])

    def to_x(a):
        return lax.ppermute(a, "shard", [(s, s ^ 2) for s in range(shards)])

    def to_y(a):
        return lax.ppermute(a, "context", [(0, 1), (1, 0)])

    def turn(a, axis):
        return jnp.concatenate(
            [
                lax.dynamic_slice_in_dim(a, jnp.bitwise_xor(me, j) * chunk, chunk, axis)
                for j in range(shards)
            ],
            axis=axis,
        )

    def around(a):
        return lax.psum(a.astype(f32), "context") - a.astype(f32)

    qkv_own = jnp.concatenate([w_query, w_key, w_value], axis=1)
    qkv_x = to_x(qkv_own)
    qkv = [qkv_own, to_core(qkv_own), qkv_x, to_core(qkv_x)]
    out_own = jnp.concatenate(
        [w_output.T, jnp.pad(w_router, ((0, 0), (0, 128 - experts)))], axis=1
    )
    out_x = to_x(out_own)
    outs = [out_own, to_core(out_own), out_x, to_core(out_x)]
    local = experts // contexts if pair else experts
    offset = here * local if pair else 0

    def mine_of(w):
        return lax.dynamic_slice_in_dim(w, offset, local, 0)

    w_own = jnp.stack([mine_of(w_gate), mine_of(w_up), mine_of(w_down).transpose(0, 2, 1)])
    w_core = to_core(w_own)
    groups = local // GROUP
    fetched = []
    for n in range(groups):
        w_x = to_x(w_own[:, n * GROUP : (n + 1) * GROUP])
        fetched.append((w_own, w_core, w_x, to_core(w_x)))

    x_low = turn(hidden.reshape(tokens, width), 1)
    g_low = turn(out_grad.reshape(tokens, width), 1)
    gain1, gain2 = turn(norm1_gain, 0), turn(norm2_gain, 0)
    positions = here * tokens + jnp.arange(tokens, dtype=jnp.int32)
    valid = (positions < seq_lengths[0]).astype(f32)[:, None]
    g_all = (g_low.astype(f32) * valid).astype(bf16)
    routes = expert_routes.reshape(tokens, expert_routes.shape[-1])
    member = jnp.any(
        routes[:, :, None] == jnp.arange(experts, dtype=jnp.int32)[None, None, :], axis=1
    ).astype(f32)
    if pair:
        g_far = to_y(
            jnp.concatenate([g_all, jnp.pad(member, ((0, 0), (0, 128 - experts))).astype(bf16)], axis=1),
        )
        g_far, member_far = g_far[:, :width], g_far[:, width : width + experts].astype(f32)
    proj, h1, rate1, squares = qkv_call(x_low, gain1, qkv)
    inv_freq = 10000.0 ** (-(2.0 * jnp.arange(HEAD_DIM // 2, dtype=f32)) / HEAD_DIM)
    angles = positions.astype(f32)[:, None] * inv_freq[None, :]
    cosine, sine = jnp.cos(angles), jnp.sin(angles)
    cosine = jnp.concatenate([cosine, cosine], axis=1)
    sine = jnp.concatenate([-sine, sine], axis=1)
    q_rot, kv, rates = rope_call(tensors, proj, squares, query_gain, key_gain, cosine, sine)
    if pair:
        kv_all = jnp.concatenate([kv, to_y(kv)], axis=0)
        base = jnp.stack([here, here, 1 - here])
    else:
        kv_all = lax.all_gather(kv, "context", axis=0, tiled=True)
        base = jnp.concatenate([here[None], jnp.arange(contexts)])
    base = (base * tokens).astype(jnp.int32)
    w_outs = [o[:, :cols] for o in outs]
    mixed, lse, attn_part = attention_call(base, q_rot, kv_all, w_outs, scale)
    w_rout = jnp.concatenate([o[:, cols : cols + experts] for o in outs], axis=0)
    h2, y1, rate2 = line_call(
        3, tensors,
        [(after_attention, attn_part, (x_low, gain2[None]), ((rows, width), (rows, 1)))],
    )

    def route(h, member):
        logits = nn(h, w_rout)
        expo_logit = jnp.exp(logits - jnp.max(logits, axis=-1, keepdims=True))
        router = expo_logit / jnp.sum(expo_logit, axis=-1, keepdims=True)
        return router, lax.dynamic_slice_in_dim(router * member, offset, local, 1)

    router, coef = route(h2, member)
    sums = dict.fromkeys(("own", "far"))
    data = {"own": (h2, g_all, coef)}
    if pair:
        h2_far = to_y(h2)
        data["far"] = (h2_far, g_far, route(h2_far, member_far)[1])
        order = [(n, t) for n in range(groups) for t in (("far", "own") if n else ("own", "far"))]
    else:
        order = [(n, "own") for n in range(groups)]
    grads, partials = None, {}
    for k, (n, t) in enumerate(order):
        final = not pair or n in partials
        done = moe_call(10 + k, n * GROUP, *data[t], fetched[n], sums[t], partials.get(n), final)
        sums[t] = done[:3]
        if not final:
            partials[n] = done[3]
            continue
        near, far = done[3], to_x(done[4])
        cuts = 2 if pair and n == 0 else 1
        for c in range(cuts):
            size = GROUP // cuts
            some = slice(c * size, (c + 1) * size)
            owned = (near[:, some].astype(f32) + far[:, some].astype(f32)).astype(bf16)
            places = offset + n * GROUP + c * size + jnp.arange(size, dtype=jnp.int32)
            if pair:
                other = to_y(owned)
                places = jnp.concatenate([places, places + local - 2 * offset])
            else:
                owned, other = lax.psum(owned.astype(f32), "context").astype(bf16), None
            grads = finish_call(places, experts, owned, other, grads)
    grad_gate, grad_up, grad_down = grads
    moe, dh, dcoef = sums["own"]
    if pair:
        moe_far, dh_far, dcoef_far = sums["far"]
        back = to_y(
            jnp.concatenate(
                [dh_far, jnp.pad(dcoef_far, ((0, 0), (0, 128 - local)))], axis=1
            ).astype(bf16),
        ).astype(f32)
        dh = dh + back[:, :width]
        far_part = back[:, width : width + local]
        dcoef = jnp.where(
            here == 0,
            jnp.concatenate([dcoef, far_part], axis=1),
            jnp.concatenate([far_part, dcoef], axis=1),
        )
        moe = moe + to_y(moe_far.astype(bf16)).astype(f32)

    def route_back(dcoef):
        dprob = dcoef * member
        return (router * (dprob - jnp.sum(router * dprob, axis=-1, keepdims=True))).astype(bf16)

    dlog = route_back(dcoef)
    dh_part = (dh + nt(dlog, w_rout)).astype(bf16)
    da, dy1, gain2_grad = line_call(
        4, tensors,
        [(after_experts, dh_part, (g_all, y1, rate2, gain2[None]), ((rows, width), (1, width)))],
    )

    def chunks_to_owner(ident, pairs):
        near = grads_call(ident, pairs)
        owned = (near[0].astype(f32) + to_x(near[1]).astype(f32)).astype(bf16)
        other = to_y(owned) if pair else around(owned)
        return owned.astype(f32) + other.astype(f32)

    sum_out = chunks_to_owner(7, [(da, mixed)])

    dqr, dkr, dvb = attention_back_call(base, da, q_rot, kv_all, lse, w_outs, scale)
    if pair:
        far = jnp.concatenate([dkr[tokens:], dvb[tokens:]], axis=1).astype(bf16)
        far = to_y(far)
    else:
        dkr, dvb = (
            lax.psum_scatter(a, "context", scatter_dimension=0, tiled=True) for a in (dkr, dvb)
        )
        far = jnp.zeros((tokens, 2 * cols), bf16)
    dqkv, gains_qk, dcoef = qk_back_call(
        tensors, dqr, dkr, dvb, far, proj, rates, query_gain, key_gain, cosine, sine, dcoef.T
    )
    dlog = jnp.pad(route_back(dcoef.T), ((0, 0), (0, 128 - experts)))
    sum_qkv = chunks_to_owner(8, [(h1, dqkv), (h2, dlog)])

    dh1_part = nt(dqkv, jnp.concatenate(qkv, axis=0)).astype(bf16)
    dx, gain1_grad, block = line_call(
        5, tensors,
        [
            (after_projections, dh1_part, (x_low, dy1, rate1, gain1[None]), ((1, width),)),
            (block_rows, moe.astype(bf16), (y1, valid), ()),
        ],
    )
    gain1_grad, gain2_grad = gain1_grad[0], gain2_grad[0]
    input_grad = turn(dx, 1).reshape(hidden.shape)
    block_out = turn(block, 1).reshape(hidden.shape)

    values = jnp.concatenate(
        [turn(gain1_grad, 0), turn(gain2_grad, 0), gains_qk[:2].reshape(-1)]
    ).reshape(-1, 128)
    sizes = (("tensor", tensors), ("shard", shards), ("context", contexts))
    gains = gains_call(sizes, 2 * width // 128, values).reshape(-1)
    gains_qk = gains[2 * width :].reshape(2, cols)
    return (
        block_out,
        input_grad,
        gains[:width],
        sum_qkv[:, :cols],
        sum_qkv[:, cols : 2 * cols],
        sum_qkv[:, 2 * cols : 3 * cols],
        gains_qk[0],
        gains_qk[1],
        sum_out.T,
        gains[width : 2 * width],
        sum_qkv[:, 3 * cols : 3 * cols + experts],
        grad_gate,
        grad_up,
        grad_down,
    )


def solution(mesh):
    in_specs = (
        P("shard", "context", None),
        P(),
        P("shard", "tensor"),
        P("shard", "tensor"),
        P("shard", "tensor"),
        P("tensor"),
        P("tensor"),
        P("tensor", "shard"),
        P(),
        P("shard", None),
        P(None, "shard", "tensor"),
        P(None, "shard", "tensor"),
        P(None, "tensor", "shard"),
        P("shard"),
        P("shard", "context", None),
        P("shard", "context", None),
    )
    out_specs = (
        P("shard", "context", None),
        P("shard", "context", None),
        P(),
        P("shard", "tensor"),
        P("shard", "tensor"),
        P("shard", "tensor"),
        P("tensor"),
        P("tensor"),
        P("tensor", "shard"),
        P(),
        P("shard", None),
        P(None, "shard", "tensor"),
        P(None, "shard", "tensor"),
        P(None, "tensor", "shard"),
    )

    return jax.shard_map(body, mesh=mesh, in_specs=in_specs, out_specs=out_specs, check_vma=False)
```

```python
import functools
import heapq

import jax
import jax.numpy as jnp
from jax import lax
from jax.experimental import pallas as pl
from jax.experimental.pallas import tpu as pltpu
from jax.sharding import PartitionSpec as P


HEAD_DIM = 128
EPSILON = 1e-05
GROUP = 4
f32 = jnp.float32
bf16 = jnp.bfloat16


def nn(a, b):
    return lax.dot_general(a, b, (((1,), (0,)), ((), ())), preferred_element_type=f32)


def nt(a, b):
    return lax.dot_general(a, b, (((1,), (1,)), ((), ())), preferred_element_type=f32)


def tn(a, b):
    return lax.dot_general(a, b, (((0,), (0,)), ((), ())), preferred_element_type=f32)


def moe_kernel(
    first, partial, final, base, count,
    h_ref, g_ref, coef_ref, w_own, w_core, w_x, w_xc, *refs,
):
    refs = list(refs)
    sums_in = [] if first else [refs.pop(0) for _ in range(3)]
    grads_in = refs.pop(0) if partial else None
    moe_ref, dh_ref, dc_ref = (refs.pop(0) for _ in range(3))
    outs = [refs.pop(0) for _ in range(2 if final else 1)]
    wbuf, wsems, *swap = refs
    step = pl.program_id(0)
    chunk = h_ref.shape[1] // 4
    slot = lax.rem(step, 2)
    before = 1 - slot

    def fetch(at, slot, act):
        for piece, src in enumerate((w_own.at[:, base + at], w_core.at[:, base + at], w_x.at[:, at], w_xc.at[:, at])):
            dst = wbuf.at[slot, :, pl.ds(piece * chunk, chunk)]
            act(pltpu.make_async_copy(src, dst, wsems.at[slot, piece]))

    if final:
        keep, send, got, send_sems, got_sems, free = swap
        me = lax.axis_index("shard")
        partner = {"shard": me + 1 - 2 * lax.rem(me, 2)}

        def swap_copy(slot):
            return pltpu.make_async_remote_copy(
                src_ref=send.at[slot],
                dst_ref=got.at[slot],
                send_sem=send_sems.at[slot],
                recv_sem=got_sems.at[slot],
                device_id=partner,
                device_id_type=pl.DeviceIdType.MESH,
            )

    @pl.when(step == 0)
    def _():
        fetch(0, 0, lambda c: c.start())
        if final:
            barrier = pltpu.get_barrier_semaphore()
            pl.semaphore_signal(
                barrier, inc=1, device_id=partner, device_id_type=pl.DeviceIdType.MESH
            )
            pl.semaphore_wait(barrier, 1)
        for i, ref in enumerate((moe_ref, dh_ref, dc_ref)):
            ref[...] = jnp.zeros_like(ref) if first else sums_in[i][...]

    @pl.when(step + 1 < count)
    def _():
        fetch(step + 1, before, lambda c: c.start())

    @pl.when(step < count)
    def _():
        fetch(step, slot, lambda c: c.wait())
        lanes = lax.broadcasted_iota(jnp.int32, coef_ref.shape, 1)
        picked = lanes == base + step
        coef = jnp.sum(jnp.where(picked, coef_ref[...], 0.0), axis=1, keepdims=True)
        wg, wu, wd = wbuf.at[slot, 0], wbuf.at[slot, 1], wbuf.at[slot, 2]
        gate = nn(h_ref[...], wg[...])
        up = nn(h_ref[...], wu[...])
        dz_plain = nn(g_ref[...], wd[...])
        sig = jax.nn.sigmoid(gate)
        act = gate * sig
        z = act * up
        z_coef = (z * coef).astype(bf16)
        dcoef = jnp.sum(z * dz_plain, axis=1, keepdims=True)
        dc_ref[...] += jnp.where(picked, dcoef, 0.0)
        dz = dz_plain * coef
        dgate = (dz * up * (sig * (1.0 + gate * (1.0 - sig)))).astype(bf16)
        dup = (dz * act).astype(bf16)
        for j in range(4):
            rows = slice(j * chunk, (j + 1) * chunk)
            moe_ref[:, rows] += nt(z_coef, wd[rows, :])
            dh_ref[:, rows] += nt(dgate, wg[rows, :]) + nt(dup, wu[rows, :])
            for i, (left, right) in enumerate(((dgate, h_ref), (dup, h_ref), (z_coef, g_ref))):
                grad = tn(left, right[:, rows])
                if partial:
                    grad = grad + grads_in[j, i, 0].astype(f32)
                if final:
                    (send if j % 2 else keep)[slot, j // 2, i] = grad.astype(bf16)
                else:
                    outs[0][j, i, 0] = grad.astype(bf16)
        if final:

            @pl.when(step >= 2)
            def _():
                pl.semaphore_wait(free, 1)

            swap_copy(slot).start()

    if final:

        @pl.when(step >= 1)
        def _():
            swap_copy(before).wait()
            for j in range(2):
                outs[j][:, 0] = (
                    keep[before, j].astype(f32) + got[before, j].astype(f32)
                ).astype(bf16)

            @pl.when(step <= count - 2)
            def _():
                pl.semaphore_signal(
                    free, inc=1, device_id=partner, device_id_type=pl.DeviceIdType.MESH
                )


def moe_call(ident, base, h, g, coef, weights, sums, grads, final):
    tokens, width = h.shape
    hidden = weights[0].shape[3]
    chunk = width // 4
    first, partial = sums is None, grads is not None

    def whole(shape):
        return pl.BlockSpec(shape, lambda i: (0,) * len(shape), pipeline_mode=pl.Buffered(1))

    def expert_block(lead):
        at = (lambda i: jnp.minimum(i, GROUP - 1)) if lead else (lambda i: jnp.maximum(i - 1, 0))
        shape = (*lead, 3, 1, hidden, chunk)
        return pl.BlockSpec(shape, lambda i: (0,) * len(lead) + (0, at(i), 0, 0))

    totals = [jax.ShapeDtypeStruct(a.shape, f32) for a in (h, h, coef)]
    scratch = [pltpu.VMEM((2, 3, width, hidden), bf16), pltpu.SemaphoreType.DMA((2, 4))]
    if final:
        scratch += [pltpu.VMEM((2, 2, 3, hidden, chunk), bf16)] * 3
        scratch += [pltpu.SemaphoreType.DMA((2,))] * 2 + [pltpu.SemaphoreType.REGULAR]
    lead = () if final else (4,)
    grad_shape = jax.ShapeDtypeStruct((*lead, 3, GROUP, hidden, chunk), bf16)
    extra = ({} if not final else {"collective_id": ident, "has_side_effects": True})
    return pl.pallas_call(
        functools.partial(moe_kernel, first, partial, final, base, GROUP),
        grid=(GROUP + 1 if final else GROUP,),
        in_specs=[whole(a.shape) for a in (h, g, coef)]
        + [pl.BlockSpec(memory_space=pl.ANY)] * 4
        + ([] if first else [whole(a.shape) for a in sums])
        + ([expert_block((4,))] if partial else []),
        out_specs=[whole(a.shape) for a in totals] + [expert_block(lead)] * (2 if final else 1),
        scratch_shapes=scratch,
        out_shape=totals + [grad_shape] * (2 if final else 1),
        compiler_params=pltpu.CompilerParams(
            dimension_semantics=("arbitrary",), vmem_limit_bytes=60 * 1024 * 1024, **extra
        ),
        cost_estimate=pl.CostEstimate(
            flops=18 * tokens * width * hidden * GROUP,
            bytes_accessed=12 * width * hidden * GROUP + 32 * tokens * width,
            transcendentals=GROUP * tokens * hidden,
        ),
    )(h, g, coef, *weights, *(() if first else sums), *((grads,) if partial else ()))


def finish_kernel(count, more, places, own_ref, *refs):
    gate_ref, up_ref, down_ref = refs[-3:]

    def put(ref):
        gate_ref[0] = ref[0, 0].astype(f32).T
        up_ref[0] = ref[1, 0].astype(f32).T
        down_ref[0] = ref[2, 0].astype(f32)

    pl.when(pl.program_id(0) < count)(lambda: put(own_ref))
    if more:
        pl.when(pl.program_id(0) >= count)(lambda: put(refs[0]))


def finish_call(places, experts, own, other, grads):
    count, hidden, chunk = own.shape[1:]
    first = grads is None
    shapes = [(experts, chunk, hidden), (experts, chunk, hidden), (experts, hidden, chunk)]
    pieces = [pl.BlockSpec((3, 1, hidden, chunk), lambda i, p: (0, jnp.minimum(i, count - 1), 0, 0))]
    if other is not None:
        pieces.append(
            pl.BlockSpec((3, 1, hidden, chunk), lambda i, p: (0, jnp.maximum(i - count, 0), 0, 0))
        )
    old = 1 + len(pieces)
    return pl.pallas_call(
        functools.partial(finish_kernel, count, other is not None),
        grid_spec=pltpu.PrefetchScalarGridSpec(
            num_scalar_prefetch=1,
            grid=(count * len(pieces),),
            in_specs=pieces + ([] if first else [pl.BlockSpec(memory_space=pl.ANY)] * 3),
            out_specs=[pl.BlockSpec((1, *s[1:]), lambda i, p: (p[i], 0, 0)) for s in shapes],
        ),
        out_shape=[jax.ShapeDtypeStruct(s, f32) for s in shapes],
        input_output_aliases={} if first else {old: 0, old + 1: 1, old + 2: 2},
        compiler_params=pltpu.CompilerParams(
            dimension_semantics=("arbitrary",), vmem_limit_bytes=24 * 1024 * 1024
        ),
        cost_estimate=pl.CostEstimate(
            flops=0, bytes_accessed=36 * count * chunk * hidden, transcendentals=0
        ),
        name="finish",
    )(places, own, *(() if other is None else (other,)), *(() if first else grads))


def qkv_kernel(x_ref, gain_ref, w0, w1, w2, w3, proj_ref, h_ref, rate_ref, sq_ref, sq_acc):
    step = pl.program_id(0)

    @pl.when(step == 0)
    def _():
        x = x_ref[...].astype(f32)
        rate = lax.rsqrt(jnp.mean(x * x, axis=-1, keepdims=True) + EPSILON)
        rate_ref[...] = rate
        h_ref[...] = (x * rate * gain_ref[...]).astype(bf16)
        sq_acc[...] = jnp.zeros_like(sq_acc)

    chunk = w0.shape[0]
    proj = sum(nn(h_ref[:, j * chunk : (j + 1) * chunk], w[...]) for j, w in enumerate((w0, w1, w2, w3)))
    proj_ref[...] = proj
    lanes = lax.broadcasted_iota(jnp.int32, sq_acc.shape, 1)
    sq_acc[...] += jnp.where(lanes == step, jnp.sum(proj * proj, axis=-1, keepdims=True), 0.0)

    @pl.when(step == 2)
    def _():
        sq_ref[...] = sq_acc[...].T[: sq_ref.shape[0]]


def qkv_call(x, gain, weights):
    tokens, width = x.shape
    chunk, cols = weights[0].shape[0], weights[0].shape[1] // 3
    return pl.pallas_call(
        qkv_kernel,
        grid=(3,),
        in_specs=[
            pl.BlockSpec((tokens, width), lambda i: (0, 0), pipeline_mode=pl.Buffered(1)),
            pl.BlockSpec((1, width), lambda i: (0, 0)),
        ]
        + [pl.BlockSpec((chunk, cols), lambda i: (0, i))] * 4,
        out_specs=[
            pl.BlockSpec((tokens, cols), lambda i: (0, i)),
            pl.BlockSpec((tokens, width), lambda i: (0, 0)),
            pl.BlockSpec((tokens, 1), lambda i: (0, 0)),
            pl.BlockSpec((8, tokens), lambda i: (0, 0)),
        ],
        scratch_shapes=[pltpu.VMEM((tokens, 128), f32)],
        out_shape=[
            jax.ShapeDtypeStruct((tokens, 3 * cols), f32),
            jax.ShapeDtypeStruct((tokens, width), bf16),
            jax.ShapeDtypeStruct((tokens, 1), f32),
            jax.ShapeDtypeStruct((8, tokens), f32),
        ],
        compiler_params=pltpu.CompilerParams(
            dimension_semantics=("arbitrary",), vmem_limit_bytes=40 * 1024 * 1024
        ),
        cost_estimate=pl.CostEstimate(
            flops=6 * tokens * width * cols, bytes_accessed=12 * width * cols, transcendentals=tokens
        ),
        name="qkv",
    )(x, gain[None], *weights)


def meet(peers):
    barrier = pltpu.get_barrier_semaphore()
    for here, place in peers:

        @pl.when(here)
        def _(place=place):
            pl.semaphore_signal(
                barrier, inc=1, device_id={"tensor": place}, device_id_type=pl.DeviceIdType.MESH
            )

    pl.semaphore_wait(barrier, sum(here.astype(jnp.int32) for here, _ in peers))


def line_plan(n, subs):
    waiting = {(z, way): [] for z in range(n) for way in (0, 1)}
    free = dict.fromkeys(waiting, 0.0)
    got, sent, events = {}, [[] for _ in range(n)], []
    message, latency = 1.0, 0.2

    def post(t, *what):
        heapq.heappush(events, (t, len(seen), what))
        seen.append(0)

    def enqueue(t, z, way, kind, b, s):
        if 0 <= z + 2 * way - 1 < n:
            waiting[z, way].append((kind, s, -abs(b - z), b))
            post(t, 0, z, way)

    seen = []
    for z, way in ((0, 1), (n - 1, 0)):
        for s in range(subs):
            for b in range(n):
                if b != z:
                    enqueue(0.0, z, way, 0, b, s)
    while events:
        t, _, (arrived, z, way, *m) = heapq.heappop(events)
        if not arrived:
            if waiting[z, way] and free[z, way] <= t:
                waiting[z, way].sort()
                kind, s, _, b = waiting[z, way].pop(0)
                free[z, way] = t + message
                sent[z].append((kind, way, b, s))
                post(t + message, 0, z, way)
                post(t + message + latency, 1, z + 2 * way - 1, way, kind, b, s)
            continue
        kind, b, s = m
        if kind or b != z:
            enqueue(t, z, way, kind, b, s)
            continue
        got[z, s] = got.get((z, s), 0) + 1
        if got[z, s] == (z > 0) + (z < n - 1):
            for w in (0, 1):
                enqueue(t, z, w, 1, z, s)
    plans = []
    for z in range(n):
        plan = []
        for kind, way, b, s in sent[z]:
            step = ("own", s) if kind and b == z else ("gather" if kind else "sum", way, b, s)
            if step not in plan:
                plan.append(step)
        plans.append(plan)
    return plans


def line_kernel(n, subs, streams, *refs):
    refs = list(refs)
    ins = [[refs.pop(0) for _ in range(1 + extra)] for _, extra, _ in streams]
    outs = [[refs.pop(0) for _ in range(1 + more)] for _, _, more in streams]
    bufs = [[refs.pop(0) for _ in range(2)] for _ in streams]
    here = lax.axis_index("tensor")
    tokens, _ = ins[0][0].shape
    block = tokens // n
    size = block // subs
    piece = min(16, size)
    for more in outs:
        for ref in more[1:]:
            if ref.shape[0] == 1:
                ref[...] = jnp.zeros_like(ref)
    meet([(here > 0, here - 1), (here < n - 1, here + 1)])

    def device(z):
        inner = (z > 0, z < n - 1)

        def copy(kind, way, b, s):
            flow, s = divmod(s, subs)
            buf, sems = bufs[flow]
            at = pl.ds(b * block + s * size, size)
            edge = z == (0 if way else n - 1)
            dst = outs[flow][0].at[at] if kind else buf.at[way, 1, at]
            src = dst if kind else ins[flow][0].at[at] if edge else buf.at[way, 0, at]
            return pltpu.make_async_remote_copy(
                src_ref=src,
                dst_ref=dst,
                send_sem=sems.at[2 * kind, way, b, s],
                recv_sem=sems.at[2 * kind + 1, way, b, s],
                device_id={"tensor": z + 2 * way - 1},
                device_id_type=pl.DeviceIdType.MESH,
            )

        def came(kind, way, b, s):
            flow, s = divmod(s, subs)
            buf, sems = bufs[flow]
            at = pl.ds(b * block + s * size, size)
            dst = outs[flow][0].at[at] if kind else buf.at[way, 1, at]
            pltpu.make_async_remote_copy(
                src_ref=dst,
                dst_ref=dst,
                send_sem=sems.at[2 * kind, way, b, s],
                recv_sem=sems.at[2 * kind + 1, way, b, s],
                device_id={"tensor": z - 2 * way + 1},
                device_id_type=pl.DeviceIdType.MESH,
            ).wait_recv()

        def own(s):
            flow, local = divmod(s, subs)
            for way in (0, 1):
                if inner[1 - way]:
                    came(0, way, z, s)

            def rows(i, _):
                at = pl.multiple_of(z * block + local * size + i * piece, piece)
                at = pl.ds(at, piece)
                total = ins[flow][0][at].astype(f32)
                for way in (0, 1):
                    if inner[1 - way]:
                        total = total + bufs[flow][0][way, 1, at].astype(f32)
                nearby = pl.ds(pl.multiple_of(local * size + i * piece, piece), piece)
                outs[flow][0][at] = streams[flow][0](total, at, nearby, ins[flow][1:], outs[flow][1:])

            lax.fori_loop(0, size // piece, rows, None)
            for way in (0, 1):
                if inner[way]:
                    copy(1, way, z, s).start()

        def add(way, b, s):
            flow, local = divmod(s, subs)
            buf, part = bufs[flow][0], ins[flow][0]

            def rows(i, _):
                at = pl.ds(pl.multiple_of(b * block + local * size + i * piece, piece), piece)
                buf[way, 0, at] = (part[at].astype(f32) + buf[way, 1, at].astype(f32)).astype(bf16)

            lax.fori_loop(0, size // piece, rows, None)

        for kind, *what in plans[z]:
            if kind == "own":
                own(*what)
                continue
            way, b, s = what
            if inner[1 - way]:
                came(kind == "gather", way, b, s)
                if kind == "sum":
                    add(way, b, s)
            copy(int(kind == "gather"), way, b, s).start()
        for s in range(subs * len(streams)):
            for b in range(n):
                for way in (0, 1):
                    if not inner[way] and ((z > b) if way else (z < b)):
                        came(1, way, b, s)
                    if (z < b) if way else (z > b):
                        copy(0, way, b, s).wait_send()
                    elif inner[way]:
                        copy(1, way, b, s).wait_send()

    plans = line_plan(n, subs * len(streams))
    for z in range(n):
        pl.when(here == z)(functools.partial(device, z))


def line_call(ident, n, streams):
    subs = 2
    vmem = pl.BlockSpec(memory_space=pltpu.VMEM)
    shapes, scratch, inputs, kinds = [], [], [], []
    for finish, part, extras, more in streams:
        tokens, width = part.shape
        kinds.append((finish, len(extras), len(more)))
        inputs += [part, *extras]
        shapes += [jax.ShapeDtypeStruct((tokens, width), bf16)]
        shapes += [jax.ShapeDtypeStruct(m, f32) for m in more]
        scratch += [
            pltpu.VMEM((2, 2, tokens, width), bf16),
            pltpu.SemaphoreType.DMA((4, 2, n, subs)),
        ]
    return pl.pallas_call(
        functools.partial(line_kernel, n, subs, kinds),
        in_specs=[vmem] * len(inputs),
        out_specs=[vmem] * len(shapes),
        out_shape=shapes,
        scratch_shapes=scratch,
        compiler_params=pltpu.CompilerParams(
            collective_id=ident, has_side_effects=True, vmem_limit_bytes=58 * 1024 * 1024
        ),
        cost_estimate=pl.CostEstimate(
            flops=12000 * tokens * width, bytes_accessed=8 * tokens * width, transcendentals=0
        ),
    )(*inputs)


def after_attention(total, whole, local, refs, more):
    x_ref, gain_ref = refs
    y_ref, rate_ref = more
    y = x_ref[whole].astype(f32) + total
    rate = lax.rsqrt(jnp.mean(y * y, axis=-1, keepdims=True) + EPSILON)
    y_ref[local] = y
    rate_ref[local] = rate
    return (y * rate * gain_ref[...]).astype(bf16)


def norm_back(total, base, x, rate, gain_ref, grad_ref):
    grad_ref[...] += jnp.sum(total * (x * rate), axis=0, keepdims=True)
    e = total * gain_ref[...]
    return base + rate * e - x * (rate * rate * rate) * jnp.mean(e * x, axis=-1, keepdims=True)


def after_experts(total, whole, local, refs, more):
    g_ref, y_ref, rate_ref, gain_ref = refs
    dy_ref, grad_ref = more
    dy = norm_back(
        total, g_ref[whole].astype(f32), y_ref[local], rate_ref[local], gain_ref, grad_ref
    )
    dy_ref[local] = dy
    return dy.astype(bf16)


def after_projections(total, whole, local, refs, more):
    x_ref, dy_ref, rate_ref, gain_ref = refs
    (grad_ref,) = more
    x = x_ref[whole].astype(f32)
    dx = norm_back(total, dy_ref[local], x, rate_ref[whole], gain_ref, grad_ref)
    return dx.astype(bf16)


def block_rows(total, whole, local, refs, more):
    y_ref, valid_ref = refs
    return (valid_ref[whole] * (y_ref[local] + total)).astype(bf16)


def exchange(n, mine_ref, got_ref, sems):
    z = lax.axis_index("tensor")
    places = [lax.rem(z + d, n) for d in range(n)]
    meet([(z >= 0, p) for p in places[1:]])
    copies = [
        pltpu.make_async_remote_copy(
            src_ref=mine_ref,
            dst_ref=got_ref.at[z],
            send_sem=sems.at[0, d],
            recv_sem=sems.at[1, d],
            device_id={"tensor": places[d]},
            device_id_type=pl.DeviceIdType.MESH,
        )
        for d in range(1, n)
    ]
    for c in copies:
        c.start()
    got_ref[z] = mine_ref[...]

    def total():
        for c in copies:
            c.wait()
        return sum(got_ref[i] for i in range(n))

    return total


def rope_kernel(n, proj_ref, sq_ref, gq_ref, gk_ref, cos_ref, sin_ref, q_ref, kv_ref, rate_ref, mine, got, sems):
    _, cols = q_ref.shape
    mine[...] = sq_ref[...]
    total = exchange(n, mine, got, sems)
    kv_ref[:, cols:] = proj_ref[:, 2 * cols :].astype(bf16)
    sums = total()
    rates = lax.rsqrt(sums / (n * cols) + EPSILON).T
    rate_ref[...] = rates
    cosine, sine = cos_ref[...], sin_ref[...]

    def turned(part, rate, gain, head):
        at = slice(head * HEAD_DIM, (head + 1) * HEAD_DIM)
        a = proj_ref[:, part * cols + head * HEAD_DIM : part * cols + (head + 1) * HEAD_DIM]
        a = a * rate * gain[:, at]
        return (a * cosine + pltpu.roll(a, HEAD_DIM // 2, 1) * sine).astype(bf16)

    for head in range(cols // HEAD_DIM):
        at = slice(head * HEAD_DIM, (head + 1) * HEAD_DIM)
        q_ref[:, at] = turned(0, rates[:, 0:1], gq_ref, head)
        kv_ref[:, at] = turned(1, rates[:, 1:2], gk_ref, head)


def exchange_scratch(n, tokens, rows=8):
    return [
        pltpu.VMEM((rows, tokens), f32),
        pltpu.VMEM((n, rows, tokens), f32),
        pltpu.SemaphoreType.DMA((2, n)),
    ]


def rope_call(n, proj, sq, gq, gk, cosine, sine):
    tokens, cols = proj.shape[0], proj.shape[1] // 3
    vmem = pl.BlockSpec(memory_space=pltpu.VMEM)
    return pl.pallas_call(
        functools.partial(rope_kernel, n),
        in_specs=[vmem] * 6,
        out_specs=[vmem] * 3,
        out_shape=[
            jax.ShapeDtypeStruct((tokens, cols), bf16),
            jax.ShapeDtypeStruct((tokens, 2 * cols), bf16),
            jax.ShapeDtypeStruct((tokens, 8), f32),
        ],
        scratch_shapes=exchange_scratch(n, tokens),
        compiler_params=pltpu.CompilerParams(
            collective_id=1, has_side_effects=True, vmem_limit_bytes=40 * 1024 * 1024
        ),
        cost_estimate=pl.CostEstimate(
            flops=2000 * tokens * cols, bytes_accessed=18 * tokens * cols, transcendentals=tokens
        ),
        name="rope",
    )(proj, sq, gq[None], gk[None], cosine, sine)


def qk_back_kernel(
    n, dq_ref, dk_ref, dv_ref, far_ref, proj_ref, rate_ref, gq_ref, gk_ref, cos_ref, sin_ref, dc_ref,
    out_ref, grad_ref, dcs_ref, dn, mine, got, sems,
):
    tokens, cols = dq_ref.shape
    cosine, sine = cos_ref[...], sin_ref[...]
    lanes = lax.broadcasted_iota(jnp.int32, (tokens, HEAD_DIM), 1)
    stats = jnp.zeros((tokens, HEAD_DIM), f32)
    rates = rate_ref[...]
    for part, gain in ((0, gq_ref), (1, gk_ref)):
        stat = jnp.zeros((tokens, 1), f32)
        rate = rates[:, part : part + 1]
        for head in range(cols // HEAD_DIM):
            at = slice(head * HEAD_DIM, (head + 1) * HEAD_DIM)
            if part:
                a = dk_ref[:, at] + far_ref[:, at].astype(f32)
            else:
                a = dq_ref[:, at]
            a = a * cosine - pltpu.roll(a, HEAD_DIM // 2, 1) * sine
            plain = proj_ref[:, part * cols + head * HEAD_DIM : part * cols + (head + 1) * HEAD_DIM]
            grad_ref[part : part + 1, at] = jnp.sum(a * plain * rate, axis=0, keepdims=True)
            a = a * gain[:, at]
            dn[part, :, at] = a
            stat += jnp.sum(a * plain, axis=-1, keepdims=True)
        stats = jnp.where(lanes == part, stat, stats)
    mine[:8] = stats.T[:8]
    mine[8:] = dc_ref[...]
    total = exchange(n, mine, got, sems)
    out_ref[:, 2 * cols :] = (dv_ref[...] + far_ref[:, cols:].astype(f32)).astype(bf16)
    whole = total()
    dcs_ref[...] = whole[8:]
    means = (whole[:8] / (n * cols)).T
    for part in (0, 1):
        rate = rates[:, part : part + 1]
        factor = rate * rate * rate * means[:, part : part + 1]
        at = slice(part * cols, (part + 1) * cols)
        out_ref[:, at] = (rate * dn[part] - proj_ref[:, at] * factor).astype(bf16)


def qk_back_call(n, dq, dk, dv, far, proj, rates, gq, gk, cosine, sine, dcoef):
    tokens, cols = dq.shape
    vmem = pl.BlockSpec(memory_space=pltpu.VMEM)
    near = pl.BlockSpec((tokens, cols), lambda i: (0, 0))
    return pl.pallas_call(
        functools.partial(qk_back_kernel, n),
        grid=(1,),
        in_specs=[vmem, near, near] + [vmem] * 8,
        out_specs=[vmem] * 3,
        out_shape=[
            jax.ShapeDtypeStruct((tokens, 3 * cols), bf16),
            jax.ShapeDtypeStruct((8, cols), f32),
            jax.ShapeDtypeStruct(dcoef.shape, f32),
        ],
        scratch_shapes=[pltpu.VMEM((2, tokens, cols), f32)]
        + exchange_scratch(n, tokens, 8 + dcoef.shape[0]),
        compiler_params=pltpu.CompilerParams(
            collective_id=2, has_side_effects=True, vmem_limit_bytes=40 * 1024 * 1024
        ),
        cost_estimate=pl.CostEstimate(
            flops=2000 * tokens * cols, bytes_accessed=30 * tokens * cols, transcendentals=0
        ),
        name="qk_back",
    )(dq, dk, dv, far, proj, rates, gq[None], gk[None], cosine, sine, dcoef)


def gains_kernel(sizes, both, in_ref, out_ref, mine, *bufs):
    mine[...] = in_ref[...]
    peers = []
    for axis, n in sizes:
        here = lax.axis_index(axis)
        peers += [(axis, d, lax.rem(here + d, n)) for d in range(1, n)]
    barrier = pltpu.get_barrier_semaphore()
    for axis, _, place in peers:
        pl.semaphore_signal(
            barrier, inc=1, device_id={axis: place}, device_id_type=pl.DeviceIdType.MESH
        )
    pl.semaphore_wait(barrier, len(peers))
    for k, (axis, n) in enumerate(sizes):
        got, sems = bufs[2 * k : 2 * k + 2]
        here = lax.axis_index(axis)
        rows = pl.ds(0, both if axis == "tensor" else mine.shape[0])
        copies = [
            pltpu.make_async_remote_copy(
                src_ref=mine.at[rows],
                dst_ref=got.at[here],
                send_sem=sems.at[0, d],
                recv_sem=sems.at[1, d],
                device_id={axis: place},
                device_id_type=pl.DeviceIdType.MESH,
            )
            for a, d, place in peers
            if a == axis
        ]
        for c in copies:
            c.start()
        got[here] = mine[rows]
        for c in copies:
            c.wait()
        mine[rows] = sum(got[i] for i in range(n))
    out_ref[...] = mine[...]


def gains_call(sizes, both, values):
    rows = values.shape[0]
    vmem = pl.BlockSpec(memory_space=pltpu.VMEM)
    scratch = [pltpu.VMEM((rows, 128), f32)]
    for axis, n in sizes:
        scratch += [
            pltpu.VMEM((n, both if axis == "tensor" else rows, 128), f32),
            pltpu.SemaphoreType.DMA((2, n)),
        ]
    return pl.pallas_call(
        functools.partial(gains_kernel, sizes, both),
        in_specs=[vmem],
        out_specs=vmem,
        out_shape=jax.ShapeDtypeStruct(values.shape, f32),
        scratch_shapes=scratch,
        compiler_params=pltpu.CompilerParams(collective_id=6, has_side_effects=True),
        cost_estimate=pl.CostEstimate(flops=10000000, bytes_accessed=100000, transcendentals=0),
        name="gains",
    )(values)


def grads_kernel(count, *refs):
    pairs = [(refs[2 * i], refs[2 * i + 1]) for i in range(count)]
    out0, out2, send, got, send_sems, got_sems = refs[2 * count :]
    me = lax.axis_index("shard")
    partner = {"shard": me + 1 - 2 * lax.rem(me, 2)}
    chunk = send.shape[1]
    barrier = pltpu.get_barrier_semaphore()
    pl.semaphore_signal(barrier, inc=1, device_id=partner, device_id_type=pl.DeviceIdType.MESH)
    pl.semaphore_wait(barrier, 1)

    def products(j, put):
        col = 0
        for left, right in pairs:
            n = right.shape[1]
            put(slice(col, col + n), tn(left[:, j * chunk : (j + 1) * chunk], right[...]))
            col += n

    copies = []
    for k, j in enumerate((1, 3)):

        def store(at, value, k=k):
            send[k, :, at] = value.astype(bf16)

        products(j, store)
        copies.append(
            pltpu.make_async_remote_copy(
                src_ref=send.at[k],
                dst_ref=got.at[k],
                send_sem=send_sems.at[k],
                recv_sem=got_sems.at[k],
                device_id=partner,
                device_id_type=pl.DeviceIdType.MESH,
            )
        )
        copies[k].start()
    for k, (j, out) in enumerate(((0, out0), (2, out2))):
        copies[k].wait_recv()

        def store(at, value, k=k, out=out):
            out[:, at] = (value + got[k, :, at].astype(f32)).astype(bf16)

        products(j, store)
    for c in copies:
        c.wait_send()


def grads_call(ident, pairs):
    tokens, width = pairs[0][0].shape
    chunk, cols = width // 4, sum(b.shape[1] for _, b in pairs)
    vmem = pl.BlockSpec(memory_space=pltpu.VMEM)
    return pl.pallas_call(
        functools.partial(grads_kernel, len(pairs)),
        in_specs=[vmem] * (2 * len(pairs)),
        out_specs=[vmem] * 2,
        out_shape=[jax.ShapeDtypeStruct((chunk, cols), bf16)] * 2,
        scratch_shapes=[pltpu.VMEM((2, chunk, cols), bf16)] * 2 + [pltpu.SemaphoreType.DMA((2,))] * 2,
        compiler_params=pltpu.CompilerParams(
            collective_id=ident, has_side_effects=True, vmem_limit_bytes=50 * 1024 * 1024
        ),
        cost_estimate=pl.CostEstimate(
            flops=2 * tokens * width * cols, bytes_accessed=4 * tokens * width, transcendentals=0
        ),
    )(*(a for p in pairs for a in p))


def masked_scores(base, q, keys, scale, flip):
    tokens = q.shape[0]
    raw = (nt(keys, q) if flip else nt(q, keys)) * scale
    axis = 0 if flip else 1
    parts = []
    for i in range(keys.shape[0] // tokens):
        rows = slice(i * tokens, (i + 1) * tokens)
        part = raw[rows] if flip else raw[:, rows]
        key_pos = base[i + 1] + lax.broadcasted_iota(jnp.int32, part.shape, axis)
        query_pos = base[0] + lax.broadcasted_iota(jnp.int32, part.shape, 1 - axis)
        parts.append(jnp.where(key_pos <= query_pos, part, -1e30))
    return jnp.concatenate(parts, axis=axis)


def attention_kernel(scale, base, q_ref, k_ref, v_ref, w0, w1, w2, w3, mixed_ref, lse_ref, part_ref, lse_acc):
    head = pl.program_id(0)
    scores = masked_scores(base, q_ref[...], k_ref[...], scale, False)
    top = jnp.max(scores, axis=-1, keepdims=True)
    expo = jnp.exp(scores - top)
    total = jnp.sum(expo, axis=-1, keepdims=True)
    mixed = nn((expo / total).astype(bf16), v_ref[...]).astype(bf16)
    for h in range(mixed_ref.shape[1] // HEAD_DIM):

        @pl.when(head == h)
        def _(h=h):
            mixed_ref[:, h * HEAD_DIM : (h + 1) * HEAD_DIM] = mixed

    @pl.when(head == 0)
    def _():
        lse_acc[...] = jnp.zeros_like(lse_acc)

    lanes = lax.broadcasted_iota(jnp.int32, lse_acc.shape, 1)
    lse_acc[...] += jnp.where(lanes == head, top + jnp.log(total), 0.0)

    @pl.when(head == pl.num_programs(0) - 1)
    def _():
        lse_ref[...] = lse_acc[...].T[: lse_ref.shape[0]]
        chunk = w0.shape[0]
        for j, w in enumerate((w0, w1, w2, w3)):
            part_ref[:, j * chunk : (j + 1) * chunk] = nt(mixed_ref[...], w[...]).astype(bf16)


def attention_call(base, q, kv, weights, scale):
    tokens, cols = q.shape
    heads, keys, chunk = cols // HEAD_DIM, kv.shape[0], weights[0].shape[0]
    return pl.pallas_call(
        functools.partial(attention_kernel, scale),
        grid_spec=pltpu.PrefetchScalarGridSpec(
            num_scalar_prefetch=1,
            grid=(heads,),
            in_specs=[
                pl.BlockSpec((tokens, HEAD_DIM), lambda h, b: (0, h)),
                pl.BlockSpec((keys, HEAD_DIM), lambda h, b: (0, h)),
                pl.BlockSpec((keys, HEAD_DIM), lambda h, b: (0, heads + h)),
            ]
            + [pl.BlockSpec((chunk, cols), lambda h, b: (0, 0), pipeline_mode=pl.Buffered(1))] * 4,
            out_specs=[
                pl.BlockSpec((tokens, cols), lambda h, b: (0, 0)),
                pl.BlockSpec((8, tokens), lambda h, b: (0, 0)),
                pl.BlockSpec((tokens, 4 * chunk), lambda h, b: (0, 0)),
            ],
            scratch_shapes=[pltpu.VMEM((tokens, 128), f32)],
        ),
        out_shape=[
            jax.ShapeDtypeStruct((tokens, cols), bf16),
            jax.ShapeDtypeStruct((8, tokens), f32),
            jax.ShapeDtypeStruct((tokens, 4 * chunk), bf16),
        ],
        compiler_params=pltpu.CompilerParams(
            dimension_semantics=("arbitrary",), vmem_limit_bytes=50 * 1024 * 1024
        ),
        cost_estimate=pl.CostEstimate(
            flops=4 * tokens * keys * cols * 4 + 8 * tokens * cols * chunk,
            bytes_accessed=8 * tokens * cols,
            transcendentals=heads * tokens * keys,
        ),
        name="attention",
    )(base, q, kv, kv, *weights)


def attention_back_kernel(
    scale, base, da_ref, q_ref, k_ref, v_ref, lse_ref, w0, w1, w2, w3, dq_ref, dk_ref, dv_ref, dmix
):
    head = pl.program_id(0)

    @pl.when(head == 0)
    def _():
        chunk = w0.shape[0]
        whole = sum(
            nn(da_ref[:, j * chunk : (j + 1) * chunk], w[...])
            for j, w in enumerate((w0, w1, w2, w3))
        ).astype(bf16)
        for h in range(dmix.shape[0]):
            dmix[h] = whole[:, h * HEAD_DIM : (h + 1) * HEAD_DIM]

    q, keys, values, dm = q_ref[...], k_ref[...], v_ref[...], dmix[head]
    scores = masked_scores(base, q, keys, scale, True)
    probs = jnp.exp(scores - lse_ref[pl.ds(head, 1), :])
    dprobs = nt(values, dm)
    ds = (probs * (dprobs - jnp.sum(probs * dprobs, axis=0, keepdims=True))).astype(bf16)
    dq_ref[...] = tn(ds, keys) * scale
    dk_ref[...] = nn(ds, q) * scale
    dv_ref[...] = nn(probs.astype(bf16), dm)


def attention_back_call(base, da, q, kv, lse, weights, scale):
    tokens, cols = q.shape
    heads, keys, chunk = cols // HEAD_DIM, kv.shape[0], weights[0].shape[0]
    return pl.pallas_call(
        functools.partial(attention_back_kernel, scale),
        grid_spec=pltpu.PrefetchScalarGridSpec(
            num_scalar_prefetch=1,
            grid=(heads,),
            in_specs=[
                pl.BlockSpec(da.shape, lambda h, b: (0, 0), pipeline_mode=pl.Buffered(1)),
                pl.BlockSpec((tokens, HEAD_DIM), lambda h, b: (0, h)),
                pl.BlockSpec((keys, HEAD_DIM), lambda h, b: (0, h)),
                pl.BlockSpec((keys, HEAD_DIM), lambda h, b: (0, heads + h)),
                pl.BlockSpec(lse.shape, lambda h, b: (0, 0)),
            ]
            + [pl.BlockSpec((chunk, cols), lambda h, b: (0, 0), pipeline_mode=pl.Buffered(1))] * 4,
            out_specs=[
                pl.BlockSpec((tokens, HEAD_DIM), lambda h, b: (0, h)),
                pl.BlockSpec((keys, HEAD_DIM), lambda h, b: (0, h)),
                pl.BlockSpec((keys, HEAD_DIM), lambda h, b: (0, h)),
            ],
            scratch_shapes=[pltpu.VMEM((heads, tokens, HEAD_DIM), bf16)],
        ),
        out_shape=[
            jax.ShapeDtypeStruct((tokens, cols), f32),
            jax.ShapeDtypeStruct((keys, cols), f32),
            jax.ShapeDtypeStruct((keys, cols), f32),
        ],
        compiler_params=pltpu.CompilerParams(
            dimension_semantics=("arbitrary",), vmem_limit_bytes=50 * 1024 * 1024
        ),
        cost_estimate=pl.CostEstimate(
            flops=10 * tokens * keys * cols + 8 * tokens * cols * chunk,
            bytes_accessed=24 * tokens * cols,
            transcendentals=heads * tokens * keys,
        ),
        name="attention_back",
    )(base, da, q, kv, kv, lse, *weights)


def body(
    hidden, norm1_gain, w_query, w_key, w_value, query_gain, key_gain, w_output,
    norm2_gain, w_router, w_gate, w_up, w_down, seq_lengths, expert_routes, out_grad,
):
    slots, tokens, width = hidden.shape
    shards, contexts, tensors = (
        lax.axis_size("shard"),
        lax.axis_size("context"),
        lax.axis_size("tensor"),
    )
    assert slots == 1 and shards == 4
    me, here = lax.axis_index("shard"), lax.axis_index("context")
    pair = contexts == 2
    chunk = width // shards
    cols = w_query.shape[1]
    experts = w_gate.shape[0]
    scale = HEAD_DIM ** (-0.5)
    rows = tokens // tensors

    def to_core(a):
        return lax.ppermute(a, "shard", [(s, s ^ 1) for s in range(shards)])

    def to_x(a):
        return lax.ppermute(a, "shard", [(s, s ^ 2) for s in range(shards)])

    def to_y(a):
        return lax.ppermute(a, "context", [(0, 1), (1, 0)])

    def turn(a, axis):
        return jnp.concatenate(
            [
                lax.dynamic_slice_in_dim(a, jnp.bitwise_xor(me, j) * chunk, chunk, axis)
                for j in range(shards)
            ],
            axis=axis,
        )

    def around(a):
        return lax.psum(a.astype(f32), "context") - a.astype(f32)

    qkv_own = jnp.concatenate([w_query, w_key, w_value], axis=1)
    qkv_x = to_x(qkv_own)
    qkv = [qkv_own, to_core(qkv_own), qkv_x, to_core(qkv_x)]
    out_own = jnp.concatenate(
        [w_output.T, jnp.pad(w_router, ((0, 0), (0, 128 - experts)))], axis=1
    )
    out_x = to_x(out_own)
    outs = [out_own, to_core(out_own), out_x, to_core(out_x)]
    local = experts // contexts if pair else experts
    offset = here * local if pair else 0

    def mine_of(w):
        return lax.dynamic_slice_in_dim(w, offset, local, 0)

    w_own = jnp.stack([mine_of(w_gate), mine_of(w_up), mine_of(w_down).transpose(0, 2, 1)])
    w_core = to_core(w_own)
    groups = local // GROUP
    fetched = []
    for n in range(groups):
        w_x = to_x(w_own[:, n * GROUP : (n + 1) * GROUP])
        fetched.append((w_own, w_core, w_x, to_core(w_x)))

    x_low = turn(hidden.reshape(tokens, width), 1)
    g_low = turn(out_grad.reshape(tokens, width), 1)
    gain1, gain2 = turn(norm1_gain, 0), turn(norm2_gain, 0)
    positions = here * tokens + jnp.arange(tokens, dtype=jnp.int32)
    valid = (positions < seq_lengths[0]).astype(f32)[:, None]
    g_all = (g_low.astype(f32) * valid).astype(bf16)
    routes = expert_routes.reshape(tokens, expert_routes.shape[-1])
    member = jnp.any(
        routes[:, :, None] == jnp.arange(experts, dtype=jnp.int32)[None, None, :], axis=1
    ).astype(f32)
    if pair:
        g_far = to_y(jnp.concatenate([g_all, jnp.pad(member, ((0, 0), (0, 128 - experts))).astype(bf16)], axis=1))
        g_far, member_far = g_far[:, :width], g_far[:, width : width + experts].astype(f32)
    proj, h1, rate1, squares = qkv_call(x_low, gain1, qkv)
    inv_freq = 10000.0 ** (-(2.0 * jnp.arange(HEAD_DIM // 2, dtype=f32)) / HEAD_DIM)
    angles = positions.astype(f32)[:, None] * inv_freq[None, :]
    cosine, sine = jnp.cos(angles), jnp.sin(angles)
    cosine = jnp.concatenate([cosine, cosine], axis=1)
    sine = jnp.concatenate([-sine, sine], axis=1)
    q_rot, kv, rates = rope_call(tensors, proj, squares, query_gain, key_gain, cosine, sine)
    if pair:
        kv_all = jnp.concatenate([kv, to_y(kv)], axis=0)
        base = jnp.stack([here, here, 1 - here])
    else:
        kv_all = lax.all_gather(kv, "context", axis=0, tiled=True)
        base = jnp.concatenate([here[None], jnp.arange(contexts)])
    base = (base * tokens).astype(jnp.int32)
    w_outs = [o[:, :cols] for o in outs]
    mixed, lse, attn_part = attention_call(base, q_rot, kv_all, w_outs, scale)
    w_rout = jnp.concatenate([o[:, cols : cols + experts] for o in outs], axis=0)
    h2, y1, rate2 = line_call(
        3, tensors,
        [(after_attention, attn_part, (x_low, gain2[None]), ((rows, width), (rows, 1)))],
    )

    def route(h, member):
        logits = nn(h, w_rout)
        expo_logit = jnp.exp(logits - jnp.max(logits, axis=-1, keepdims=True))
        router = expo_logit / jnp.sum(expo_logit, axis=-1, keepdims=True)
        return router, lax.dynamic_slice_in_dim(router * member, offset, local, 1)

    router, coef = route(h2, member)
    sums = dict.fromkeys(("own", "far"))
    data = {"own": (h2, g_all, coef)}
    if pair:
        h2_far = to_y(h2)
        data["far"] = (h2_far, g_far, route(h2_far, member_far)[1])
        order = [(n, t) for n in range(groups) for t in (("far", "own") if n else ("own", "far"))]
    else:
        order = [(n, "own") for n in range(groups)]
    grads, partials = None, {}
    for k, (n, t) in enumerate(order):
        final = not pair or n in partials
        done = moe_call(
            10 + k, n * GROUP, *data[t], fetched[n], sums[t], partials.get(n), final
        )
        sums[t] = done[:3]
        if not final:
            partials[n] = done[3]
            continue
        near, far = done[3], to_x(done[4])
        cuts = 2 if pair and n == 0 else 1
        for c in range(cuts):
            size = GROUP // cuts
            some = slice(c * size, (c + 1) * size)
            owned = (near[:, some].astype(f32) + far[:, some].astype(f32)).astype(bf16)
            places = offset + n * GROUP + c * size + jnp.arange(size, dtype=jnp.int32)
            if pair:
                other = to_y(owned)
                places = jnp.concatenate([places, places + local - 2 * offset])
            else:
                owned, other = lax.psum(owned.astype(f32), "context").astype(bf16), None
            grads = finish_call(places, experts, owned, other, grads)
    grad_gate, grad_up, grad_down = grads
    moe, dh, dcoef = sums["own"]
    if pair:
        moe_far, dh_far, dcoef_far = sums["far"]
        back = to_y(
            jnp.concatenate(
                [dh_far, jnp.pad(dcoef_far, ((0, 0), (0, 128 - local)))], axis=1
            ).astype(bf16),
        ).astype(f32)
        dh = dh + back[:, :width]
        far_part = back[:, width : width + local]
        dcoef = jnp.where(
            here == 0,
            jnp.concatenate([dcoef, far_part], axis=1),
            jnp.concatenate([far_part, dcoef], axis=1),
        )
        moe = moe + to_y(moe_far.astype(bf16)).astype(f32)

    def route_back(dcoef):
        dprob = dcoef * member
        return (router * (dprob - jnp.sum(router * dprob, axis=-1, keepdims=True))).astype(bf16)

    dlog = route_back(dcoef)
    dh_part = (dh + nt(dlog, w_rout)).astype(bf16)
    da, dy1, gain2_grad = line_call(
        4, tensors,
        [(after_experts, dh_part, (g_all, y1, rate2, gain2[None]), ((rows, width), (1, width)))],
    )

    def chunks_to_owner(ident, pairs):
        near = grads_call(ident, pairs)
        owned = (near[0].astype(f32) + to_x(near[1]).astype(f32)).astype(bf16)
        other = to_y(owned) if pair else around(owned)
        return owned.astype(f32) + other.astype(f32)

    sum_out = chunks_to_owner(7, [(da, mixed)])

    dqr, dkr, dvb = attention_back_call(base, da, q_rot, kv_all, lse, w_outs, scale)
    if pair:
        far = jnp.concatenate([dkr[tokens:], dvb[tokens:]], axis=1).astype(bf16)
        far = to_y(far)
    else:
        dkr, dvb = (
            lax.psum_scatter(a, "context", scatter_dimension=0, tiled=True) for a in (dkr, dvb)
        )
        far = jnp.zeros((tokens, 2 * cols), bf16)
    dqkv, gains_qk, dcoef = qk_back_call(
        tensors, dqr, dkr, dvb, far, proj, rates, query_gain, key_gain, cosine, sine, dcoef.T
    )
    dlog = jnp.pad(route_back(dcoef.T), ((0, 0), (0, 128 - experts)))
    sum_qkv = chunks_to_owner(8, [(h1, dqkv), (h2, dlog)])

    dh1_part = nt(dqkv, jnp.concatenate(qkv, axis=0)).astype(bf16)
    dx, gain1_grad, block = line_call(
        5, tensors,
        [
            (after_projections, dh1_part, (x_low, dy1, rate1, gain1[None]), ((1, width),)),
            (block_rows, moe.astype(bf16), (y1, valid), ()),
        ],
    )
    gain1_grad, gain2_grad = gain1_grad[0], gain2_grad[0]
    input_grad = turn(dx, 1).reshape(hidden.shape)
    block_out = turn(block, 1).reshape(hidden.shape)

    values = jnp.concatenate(
        [turn(gain1_grad, 0), turn(gain2_grad, 0), gains_qk[:2].reshape(-1)]
    ).reshape(-1, 128)
    sizes = (("tensor", tensors), ("shard", shards), ("context", contexts))
    gains = gains_call(sizes, 2 * width // 128, values).reshape(-1)
    gains_qk = gains[2 * width :].reshape(2, cols)
    return (
        block_out,
        input_grad,
        gains[:width],
        sum_qkv[:, :cols],
        sum_qkv[:, cols : 2 * cols],
        sum_qkv[:, 2 * cols : 3 * cols],
        gains_qk[0],
        gains_qk[1],
        sum_out.T,
        gains[width : 2 * width],
        sum_qkv[:, 3 * cols : 3 * cols + experts],
        grad_gate,
        grad_up,
        grad_down,
    )


def solution(mesh):
    in_specs = (
        P("shard", "context", None),
        P(),
        P("shard", "tensor"),
        P("shard", "tensor"),
        P("shard", "tensor"),
        P("tensor"),
        P("tensor"),
        P("tensor", "shard"),
        P(),
        P("shard", None),
        P(None, "shard", "tensor"),
        P(None, "shard", "tensor"),
        P(None, "tensor", "shard"),
        P("shard"),
        P("shard", "context", None),
        P("shard", "context", None),
    )
    out_specs = (
        P("shard", "context", None),
        P("shard", "context", None),
        P(),
        P("shard", "tensor"),
        P("shard", "tensor"),
        P("shard", "tensor"),
        P("tensor"),
        P("tensor"),
        P("tensor", "shard"),
        P(),
        P("shard", None),
        P(None, "shard", "tensor"),
        P(None, "shard", "tensor"),
        P(None, "tensor", "shard"),
    )

    return jax.shard_map(body, mesh=mesh, in_specs=in_specs, out_specs=out_specs, check_vma=False)
```
